32 devices in a mesh: prompts: 1 (over z), model: 4 (over y), resp: 8 (over x, core).
Axes of the slice: x: 4, y: 4, z: 1, core: 2. Of those that a mesh axis runs over, the one named last changes fastest.
The devices are a block of a 4x4x8 slice.
Arguments:
- x_prompt: bfloat16 [2048, 2048], P(('prompts', 'resp'))
- x_resp: bfloat16 [8, 1024, 2048], P(('prompts', 'resp'))
- targets: int32 [8, 1024], P(('prompts', 'resp'))
- resp_lens: int32 [8], P(('prompts', 'resp'))
- attn_gain: float32 [2, 2048], replicated
- w_query: bfloat16 [2, 2048, 16, 128], P(None, None, 'model')
- w_key: bfloat16 [2, 2048, 16, 128], P(None, None, 'model')
- w_value: bfloat16 [2, 2048, 16, 128], P(None, None, 'model')
- w_out: bfloat16 [2, 16, 128, 2048], P(None, 'model')
- mlp_gain: float32 [2, 2048], replicated
- w_gate: bfloat16 [2, 2048, 5504], P(None, None, 'model')
- w_up: bfloat16 [2, 2048, 5504], P(None, None, 'model')
- w_down: bfloat16 [2, 5504, 2048], P(None, 'model')
- final_gain: float32 [2048], replicated
- w_vocab: bfloat16 [2048, 32768], P(None, 'model')
Outputs:
- output: float32 [8, 1024], P(('prompts', 'resp'))
All inputs are finite; a program needn't handle non-finite values.
Results may differ from the reference program's by a relative error of at most 0.00244122.
Values are sent between devices in bfloat16 or wider.
A program may use at most 768 MiB of HBM per device.

```python
import jax
import jax.numpy as jnp
from jax import lax

MODEL_DIM = 2048
NUM_HEADS = 16
KV_HEADS = 16
HEAD_DIM = 128
FFN_DIM = 5504
VOCAB_SIZE = 32768
GROUP_SIZE = 8
PROMPT_ROWS = 256
RESP_LEN = 1024
LAYERS = 2
PROMPT_LEN = GROUP_SIZE * PROMPT_ROWS
EPS = 1e-6
ROPE_BASE = 10000.0


def rms_norm(acts_in, gain_vec):
    acts_f = acts_in.astype(jnp.float32)
    inv_rms = lax.rsqrt(jnp.mean(acts_f * acts_f, axis=-1, keepdims=True) + EPS)
    return (acts_f * inv_rms * gain_vec).astype(jnp.bfloat16)


def rotary(projected, positions):
    half_dim = projected.shape[-1] // 2
    frequency = ROPE_BASE ** (-jnp.arange(half_dim, dtype=jnp.float32) / half_dim)
    angles = positions.astype(jnp.float32)[..., None] * frequency
    cos_part = jnp.cos(angles)[..., None, :]
    sin_part = jnp.sin(angles)[..., None, :]
    lower_half = projected[..., :half_dim]
    upper_half = projected[..., half_dim:]
    return jnp.concatenate([lower_half * cos_part - upper_half * sin_part, upper_half * cos_part + lower_half * sin_part], axis=-1)


def attend(queries, keys, values, query_pos, key_pos):
    tokens = queries.shape[0]
    grouped = queries.reshape(tokens, KV_HEADS, NUM_HEADS // KV_HEADS, HEAD_DIM).astype(jnp.float32)
    scores = jnp.einsum('tkrd,skd->krts', grouped, keys.astype(jnp.float32)) * (HEAD_DIM ** -0.5)
    visible = key_pos[None, :] <= query_pos[:, None]
    scores = jnp.where(visible, scores, -jnp.inf)
    row_max = jnp.max(scores, axis=-1, keepdims=True)
    exp_scores = jnp.exp(scores - row_max)
    row_sum = jnp.moveaxis(jnp.sum(exp_scores, axis=-1), -1, 0)
    mixed = jnp.einsum('krts,skd->tkrd', exp_scores.astype(jnp.bfloat16).astype(jnp.float32), values.astype(jnp.float32))
    return (mixed / row_sum[..., None]).reshape(tokens, NUM_HEADS * HEAD_DIM).astype(jnp.bfloat16)


def setup_inputs(seed: int = 0, part: int = 0) -> dict:
    root_keys = jax.random.split(jax.random.key(seed), 2)
    part_keys = jax.random.split(jax.random.fold_in(root_keys[0], part), 7)
    shared_keys = jax.random.split(root_keys[1], 11)

    def normal_weight(key_in, shape, scale):
        return (jax.random.normal(key_in, shape, jnp.float32) * scale).astype(jnp.bfloat16)

    def gain_draw(key_in, shape):
        return jax.random.uniform(key_in, shape, jnp.float32, 0.25, 1.75)

    topics = jax.random.normal(part_keys[0], (4, 1, MODEL_DIM), jnp.float32)
    prompt_noise = jax.random.normal(part_keys[1], (4, PROMPT_LEN // 4, MODEL_DIM), jnp.float32)
    x_prompt = (0.6 * topics + 0.3 * prompt_noise).reshape(PROMPT_LEN, MODEL_DIM).astype(jnp.bfloat16)
    resp_topics = jax.random.normal(part_keys[2], (GROUP_SIZE, 1, MODEL_DIM), jnp.float32)
    resp_noise = jax.random.normal(part_keys[3], (GROUP_SIZE, RESP_LEN, MODEL_DIM), jnp.float32)
    x_resp = (0.6 * resp_topics + 0.3 * resp_noise).astype(jnp.bfloat16)
    targets = jax.random.randint(part_keys[4], (GROUP_SIZE, RESP_LEN), 0, VOCAB_SIZE, dtype=jnp.int32)
    targets = targets.at[0, 0].set(0).at[0, 1].set(VOCAB_SIZE - 1)
    drawn_lens = jax.random.randint(part_keys[5], (GROUP_SIZE,), RESP_LEN // 8, RESP_LEN + 1, dtype=jnp.int32)
    full_slot = jax.random.randint(part_keys[6], (), 0, GROUP_SIZE, dtype=jnp.int32)
    resp_lens = jnp.where(jnp.arange(GROUP_SIZE) == full_slot, RESP_LEN, drawn_lens).astype(jnp.int32)
    return {
        'x_prompt': x_prompt,
        'x_resp': x_resp,
        'targets': targets,
        'resp_lens': resp_lens,
        'attn_gain': gain_draw(shared_keys[0], (LAYERS, MODEL_DIM)),
        'w_query': normal_weight(shared_keys[1], (LAYERS, MODEL_DIM, NUM_HEADS, HEAD_DIM), MODEL_DIM ** -0.5),
        'w_key': normal_weight(shared_keys[2], (LAYERS, MODEL_DIM, KV_HEADS, HEAD_DIM), MODEL_DIM ** -0.5),
        'w_value': normal_weight(shared_keys[3], (LAYERS, MODEL_DIM, KV_HEADS, HEAD_DIM), MODEL_DIM ** -0.5),
        'w_out': normal_weight(shared_keys[4], (LAYERS, NUM_HEADS, HEAD_DIM, MODEL_DIM), (NUM_HEADS * HEAD_DIM) ** -0.5),
        'mlp_gain': gain_draw(shared_keys[5], (LAYERS, MODEL_DIM)),
        'w_gate': normal_weight(shared_keys[6], (LAYERS, MODEL_DIM, FFN_DIM), MODEL_DIM ** -0.5),
        'w_up': normal_weight(shared_keys[7], (LAYERS, MODEL_DIM, FFN_DIM), MODEL_DIM ** -0.5),
        'w_down': normal_weight(shared_keys[8], (LAYERS, FFN_DIM, MODEL_DIM), FFN_DIM ** -0.5),
        'final_gain': gain_draw(shared_keys[9], (MODEL_DIM,)),
        'w_vocab': normal_weight(shared_keys[10], (MODEL_DIM, VOCAB_SIZE), 2.0 * MODEL_DIM ** -0.5),
    }


def reference(x_prompt, x_resp, targets, resp_lens, attn_gain, w_query, w_key, w_value, w_out, mlp_gain, w_gate, w_up, w_down, final_gain, w_vocab):
    prompt_pos = jnp.arange(PROMPT_LEN)
    resp_pos = PROMPT_LEN + jnp.arange(RESP_LEN)
    key_pos = jnp.concatenate([prompt_pos, resp_pos])

    def project(hidden, weight, heads):
        flat = jnp.dot(hidden, weight.reshape(MODEL_DIM, heads * HEAD_DIM), preferred_element_type=jnp.float32)
        return flat.reshape(hidden.shape[0], heads, HEAD_DIM)

    def key_value(hidden, layer_idx, positions):
        keys = rotary(project(hidden, w_key[layer_idx], KV_HEADS), positions).astype(jnp.bfloat16)
        values = project(hidden, w_value[layer_idx], KV_HEADS).astype(jnp.bfloat16)
        return keys, values

    def query_proj(hidden, layer_idx, positions):
        return rotary(project(hidden, w_query[layer_idx], NUM_HEADS), positions).astype(jnp.bfloat16)

    def finish(residual, mixed, layer_idx):
        attn_out = jnp.dot(mixed, w_out[layer_idx].reshape(NUM_HEADS * HEAD_DIM, MODEL_DIM), preferred_element_type=jnp.float32)
        residual = (residual.astype(jnp.float32) + attn_out).astype(jnp.bfloat16)
        hidden = rms_norm(residual, mlp_gain[layer_idx])
        gate = jnp.dot(hidden, w_gate[layer_idx], preferred_element_type=jnp.float32)
        up_proj = jnp.dot(hidden, w_up[layer_idx], preferred_element_type=jnp.float32)
        inner = (jax.nn.silu(gate) * up_proj).astype(jnp.bfloat16)
        down_out = jnp.dot(inner, w_down[layer_idx], preferred_element_type=jnp.float32)
        return (residual.astype(jnp.float32) + down_out).astype(jnp.bfloat16)

    residual = x_prompt
    prompt_cache = []
    for layer_idx in range(LAYERS):
        hidden = rms_norm(residual, attn_gain[layer_idx])
        keys, values = key_value(hidden, layer_idx, prompt_pos)
        prompt_cache.append((keys, values))
        if layer_idx < LAYERS - 1:
            blocks = query_proj(hidden, layer_idx, prompt_pos).reshape(GROUP_SIZE, PROMPT_ROWS, NUM_HEADS, HEAD_DIM)
            block_pos = prompt_pos.reshape(GROUP_SIZE, PROMPT_ROWS)
            mixed = lax.map(lambda block_args: attend(block_args[0], keys, values, block_args[1], prompt_pos), (blocks, block_pos))
            residual = finish(residual, mixed.reshape(PROMPT_LEN, NUM_HEADS * HEAD_DIM), layer_idx)

    def one_response(resp_args):
        residual_r, target_row, length = resp_args
        for layer_idx in range(LAYERS):
            hidden = rms_norm(residual_r, attn_gain[layer_idx])
            keys, values = key_value(hidden, layer_idx, resp_pos)
            queries = query_proj(hidden, layer_idx, resp_pos)
            all_keys = jnp.concatenate([prompt_cache[layer_idx][0], keys], axis=0)
            all_values = jnp.concatenate([prompt_cache[layer_idx][1], values], axis=0)
            mixed = attend(queries, all_keys, all_values, resp_pos, key_pos)
            residual_r = finish(residual_r, mixed, layer_idx)
        logits = jnp.dot(rms_norm(residual_r, final_gain), w_vocab, preferred_element_type=jnp.float32)
        picked = jnp.take_along_axis(logits, target_row[:, None], axis=-1)[:, 0]
        log_probs = picked - jax.nn.logsumexp(logits, axis=-1)
        return jnp.where(jnp.arange(RESP_LEN) < length, log_probs, 0.0)

    return lax.map(one_response, (x_resp, targets, resp_lens))
```

```python
import functools

import jax
import jax.numpy as jnp
from jax import lax
from jax.experimental import pallas as pl
from jax.experimental.pallas import tpu as pltpu
from jax.sharding import PartitionSpec as P

EPS = 1e-6
ROPE_BASE = 10000.0
LOG2E = 1.4426950408889634
VMEM_BYTES = 67043328
ROWS = 64
BF = jnp.bfloat16
F32 = jnp.float32
ANY = pl.BlockSpec(memory_space=pl.ANY)
VM = pl.BlockSpec(memory_space=pltpu.VMEM)


def remote(src, dst, send, recv, axis, where):
    return pltpu.make_async_remote_copy(src_ref=src, dst_ref=dst, send_sem=send, recv_sem=recv, device_id={axis: where}, device_id_type=pl.DeviceIdType.MESH)


def entry_barrier(peers):
    barrier = pltpu.get_barrier_semaphore()
    for axis, where in peers:
        pl.semaphore_signal(barrier, inc=1, device_id={axis: where}, device_id_type=pl.DeviceIdType.MESH)
    pl.semaphore_wait(barrier, len(peers))


def ds(start, size):
    return pl.ds(pl.multiple_of(start, size), size)


def dot(a, b):
    return jnp.dot(a, b, preferred_element_type=F32)


class Gather:
    def __init__(self, buf, send, recv, me):
        self.buf, self.send, self.recv, self.me = buf, send, recv, me
        self.right, self.left = lax.rem(me + 1, 4), lax.rem(me + 3, 4)
        self.opp = lax.rem(me + 2, 4)
        self.half = buf.shape[2] // 2

    def _copy(self, kind, c, block):
        ref = self.buf.at[c, block]
        if kind == 2:
            ref = ref.at[pl.ds(0, self.half)]
        if kind == 3:
            ref = ref.at[pl.ds(self.half, self.half)]
        return remote(ref, ref, self.send.at[kind, c], self.recv.at[kind, c], 'model', self.right if kind in (0, 2) else self.left)

    def start(self, c):
        self._copy(0, c, self.me).start()
        self._copy(1, c, self.me).start()

    def forward(self, c):
        self._copy(0, c, self.left).wait_recv()
        self._copy(2, c, self.left).start()
        self._copy(1, c, self.right).wait_recv()
        self._copy(3, c, self.right).start()

    def finish(self, c):
        self._copy(2, c, self.opp).wait_recv()
        self._copy(3, c, self.opp).wait_recv()

    def drain(self, c):
        self._copy(0, c, self.me).wait_send()
        self._copy(1, c, self.me).wait_send()
        self._copy(2, c, self.left).wait_send()
        self._copy(3, c, self.right).wait_send()


def norm_rows(src, dst, gain_ref, rows, width, tile=256):
    def square(n, total):
        block = src(ds(n * tile, tile)).astype(F32)
        sq = block * block
        for i in range(tile // 128):
            total = total + sq[:, i * 128:(i + 1) * 128]
        return total

    total = lax.fori_loop(0, width // tile, square, jnp.zeros((rows, 128), F32))
    inv = lax.rsqrt(jnp.sum(total, axis=-1, keepdims=True) * (1.0 / width) + EPS)

    def scale(n, carry):
        cols = ds(n * tile, tile)
        dst(cols, (src(cols).astype(F32) * inv * gain_ref[:, cols]).astype(BF))
        return carry

    lax.fori_loop(0, width // tile, scale, 0)


def attention_kernel(first, chunks, width, scale, *refs):
    if first:
        (xp, xr, gain, wq, wk, wv, cos, sin, o_out, x_v, h_v, q_v, k_v, v_v, kp_v, vp_v, acc_v, m_v, l_v, o_v, load, gs, gr, ks, kr, os_, or_) = refs
    else:
        (hin, wq, wk, wv, cos, sin, o_out, h_v, q_v, k_v, v_v, kp_v, vp_v, acc_v, m_v, l_v, o_v, load, gs, gr, ks, kr, os_, or_) = refs
    me = lax.axis_index('model')
    r = lax.axis_index('resp')
    chip = r // 2
    partner = r + 1 - 2 * lax.rem(r, 2)
    xs = [lax.rem(r + 2, 8), lax.rem(r + 6, 8), lax.rem(r + 4, 8)]
    gather = None if first else Gather(h_v, gs, gr, me)
    q_rows = chunks * 256 if first else (chunks - 1) * 256
    head_dim = 128
    heads = width // head_dim
    log_scale = scale * LOG2E

    loads = []
    if first:
        loads.append(pltpu.make_async_copy(xp, x_v.at[0], load.at[0]))
        for c in range(1, chunks):
            loads.append(pltpu.make_async_copy(xr.at[0, pl.ds((c - 1) * 256, 256)], x_v.at[c], load.at[c]))
    else:
        for c in range(chunks):
            loads.append(pltpu.make_async_copy(hin.at[c], h_v.at[c, me], load.at[c]))
    for cp in loads:
        cp.start()
    entry_barrier([('model', lax.rem(me + k, 4)) for k in (1, 2, 3)] + [('resp', partner)] + [('resp', x) for x in xs])

    def project(c, with_q):
        base = c * 256
        cs, sn = cos[pl.ds(base, 256), :], sin[pl.ds(base, 256), :]

        def rope(y):
            return y * cs + pltpu.roll(y, 64, 1) * sn

        h = h_v.at[c]
        for which, w in enumerate((wk, wv, wq)):
            if which == 2 and not with_q:
                continue
            for n in range(width // 256):
                y = dot(h[...].reshape(256, h.shape[-1]), w[:, pl.ds(n * 256, 256)])
                for i in range(2):
                    part = y[:, i * 128:(i + 1) * 128]
                    if which != 1:
                        part = rope(part)
                    part = part.astype(BF)
                    cols = pl.ds(n * 256 + i * 128, 128)
                    if which == 2:
                        q_v[pl.ds(base - (0 if first else 256), 256), cols] = part
                    elif c == 0:
                        (kp_v, vp_v)[which][r, :, cols] = part
                    else:
                        (k_v, v_v)[which][pl.ds(base - 256, 256), cols] = part

    def kv_copy(which, kind, block):
        ref = (kp_v, vp_v)[which].at[block]
        where = xs[kind] if kind < 3 else partner
        return remote(ref, ref, ks.at[which, kind], kr.at[which, kind], 'resp', where)

    origin = [xs[1], xs[0], xs[2]]
    other = [lax.rem(o + 8 + 1 - 2 * lax.rem(o, 2), 8) for o in origin]

    def kv_start():
        for which in range(2):
            for kind in (3, 0, 1, 2):
                kv_copy(which, kind, r).start()

    def kv_pass(kind):
        for which in range(2):
            kv_copy(which, kind, origin[kind]).wait_recv()
            kv_copy(which, 4 + kind, origin[kind]).start()

    def kv_wait(kind, block):
        for which in range(2):
            kv_copy(which, kind, block).wait_recv()

    if first:
        for c in range(chunks):
            loads[c].wait()
            norm_rows(lambda cols, c=c: x_v[c, :, cols], lambda cols, val, c=c: h_v.__setitem__((c, slice(None), cols), val), gain, 256, x_v.shape[-1])
            project(c, True)
            if c == 0:
                kv_start()
    else:
        loads[0].wait()
        gather.start(0)
        loads[1].wait()
        gather.start(1)
        for c in range(chunks + 1):
            if c < chunks:
                gather.forward(c)
                if c + 2 < chunks:
                    loads[c + 2].wait()
                    gather.start(c + 2)
            if c > 0:
                gather.finish(c - 1)
                project(c - 1, c > 1)
                if c == 1:
                    kv_start()

    rows_i = lax.broadcasted_iota(jnp.int32, (256, 256), 0)
    cols_i = lax.broadcasted_iota(jnp.int32, (256, 256), 1)
    causal = cols_i <= rows_i

    def step(q, k, v, m, l, acc, mask=False):
        s = lax.dot_general(q, k, (((1,), (1,)), ((), ())), preferred_element_type=F32)
        if mask:
            s = jnp.where(causal, s, -jnp.inf)
        m_new = jnp.maximum(m, jnp.max(s, axis=-1, keepdims=True))
        p = jnp.exp2((s - m_new) * log_scale)
        alpha = jnp.exp2((m - m_new) * log_scale)
        l = l * alpha + jnp.sum(p, axis=-1, keepdims=True)
        acc = acc * alpha + dot(p.astype(BF), v)
        return m_new, l, acc

    def load_state(row, n):
        return m_v[n, pl.ds(row, 256), 0:1], l_v[n, pl.ds(row, 256), 0:1], acc_v[pl.ds(row, 256), pl.ds(n * 128, 128)]

    def save_state(row, n, state):
        m, l, acc = state
        m_v[n, pl.ds(row, 256), :] = jnp.broadcast_to(m, (256, 128))
        l_v[n, pl.ds(row, 256), :] = jnp.broadcast_to(l, (256, 128))
        acc_v[pl.ds(row, 256), pl.ds(n * 128, 128)] = acc

    def fresh():
        return jnp.full((256, 1), -jnp.inf, F32), jnp.zeros((256, 1), F32), jnp.zeros((256, 128), F32)

    def chip_keys(x, n):
        cols = pl.ds(n * 128, 128)
        return (kp_v[pl.ds(2 * x, 2), :, cols].reshape(512, 128), vp_v[pl.ds(2 * x, 2), :, cols].reshape(512, 128))

    base_q = 256 if first else 0
    def own(j, carry):
        row = pl.multiple_of(j * 256, 256)
        for n in range(heads):
            cols = pl.ds(n * 128, 128)
            q = q_v[pl.ds(base_q + row, 256), cols]
            state = step(q, k_v[pl.ds(row, 256), cols], v_v[pl.ds(row, 256), cols], *fresh(), mask=True)

            def before(b, state, q=q, cols=cols):
                keys = ds(b * 256, 256)
                return step(q, k_v[keys, cols], v_v[keys, cols], *state)

            state = lax.fori_loop(0, j, before, state)
            save_state(base_q + row, n, state)
        return carry

    lax.fori_loop(0, chunks - 1, own, 0)

    if first:
        for n in range(heads):
            cols = pl.ds(n * 128, 128)
            save_state(0, n, step(q_v[pl.ds(0, 256), cols], kp_v[r, :, cols], vp_v[r, :, cols], *fresh(), mask=True))

    kv_pass(0)
    kv_pass(1)
    kv_wait(3, partner)
    kv_pass(2)
    if first:
        @pl.when(partner < r)
        def _():
            for n in range(heads):
                cols = pl.ds(n * 128, 128)
                save_state(0, n, step(q_v[pl.ds(0, 256), cols], kp_v[partner, :, cols], vp_v[partner, :, cols], *load_state(0, n)))

    for kind in range(3):
        kv_wait(4 + kind, other[kind])

    def o_copy(c, k):
        owner = lax.rem(me + k, 4)
        dst = o_out.at[c, :, ds(me * width, width)]
        return remote(o_v.at[c, owner], dst, os_.at[k - 1, c], or_.at[k - 1, c], 'model', owner)

    def own_copy(c):
        return pltpu.make_async_copy(o_v.at[c, me], o_out.at[c, :, ds(me * width, width)], load.at[c])

    def emit(c, n, state):
        m, l, acc = state
        out = (acc / l).astype(BF)
        for b in range(4):
            o_v[c, b, :, pl.ds(n * 128, 128)] = out[b * ROWS:(b + 1) * ROWS]

    def send(c):
        for k in (2, 1, 3):
            o_copy(c, k).start()
        own_copy(c).start()

    if first:
        for n in range(heads):
            def earlier(x, state, n=n):
                k, v = chip_keys(x, n)
                return step(q_v[pl.ds(0, 256), pl.ds(n * 128, 128)], k, v, *state)
            emit(0, n, lax.fori_loop(0, chip, earlier, load_state(0, n)))
        send(0)

    out_chunks = chunks if first else chunks - 1
    for c in range(1 if first else 0, out_chunks):
        row = c * 256
        for n in range(heads):
            q = q_v[pl.ds(row, 256), pl.ds(n * 128, 128)]

            def prompt(x, state, q=q, n=n):
                k, v = chip_keys(x, n)
                return step(q, k, v, *state)
            emit(c, n, lax.fori_loop(0, 4, prompt, load_state(row, n)))
        send(c)

    for c in range(out_chunks):
        for k in (1, 2, 3):
            o_copy(c, k).wait_recv()
            o_copy(c, k).wait_send()
        own_copy(c).wait()
    for which in range(2):
        for kind in range(7):
            kv_copy(which, kind, r if kind < 4 else origin[kind - 4]).wait_send()
    if not first:
        for c in range(chunks):
            gather.drain(c)


def attention(first, collective, hidden, gain, wq, wk, wv, cos, sin):
    width = wq.shape[-1]
    model_dim = wq.shape[0]
    chunks = 5
    outs = chunks if first else chunks - 1
    scale = 128 ** -0.5
    scratch = []
    if first:
        scratch.append(pltpu.VMEM((chunks, 256, model_dim), BF))
        scratch.append(pltpu.VMEM((chunks, 256, model_dim), BF))
    else:
        scratch.append(pltpu.VMEM((chunks, 4, ROWS, model_dim), BF))
    scratch += [
        pltpu.VMEM((outs * 256, width), BF),
        pltpu.VMEM((1024, width), BF),
        pltpu.VMEM((1024, width), BF),
        pltpu.VMEM((8, 256, width), BF),
        pltpu.VMEM((8, 256, width), BF),
        pltpu.VMEM((outs * 256, width), F32),
        pltpu.VMEM((width // 128, outs * 256, 128), F32),
        pltpu.VMEM((width // 128, outs * 256, 128), F32),
        pltpu.VMEM((outs, 4, ROWS, width), BF),
        pltpu.SemaphoreType.DMA((chunks,)),
        pltpu.SemaphoreType.DMA((4, chunks)),
        pltpu.SemaphoreType.DMA((4, chunks)),
        pltpu.SemaphoreType.DMA((2, 7)),
        pltpu.SemaphoreType.DMA((2, 7)),
        pltpu.SemaphoreType.DMA((3, outs)),
        pltpu.SemaphoreType.DMA((3, outs)),
    ]
    args = (*hidden, gain, wq, wk, wv, cos, sin) if first else (*hidden, wq, wk, wv, cos, sin)
    specs = [ANY] * len(hidden) + [VM] * (len(args) - len(hidden))
    return pl.pallas_call(
        functools.partial(attention_kernel, first, chunks, width, scale),
        name=f'attention{collective}',
        out_shape=jax.ShapeDtypeStruct((outs, ROWS, 4 * width), BF),
        in_specs=specs,
        out_specs=ANY,
        scratch_shapes=scratch,
        compiler_params=pltpu.CompilerParams(collective_id=collective, has_side_effects=True, vmem_limit_bytes=VMEM_BYTES),
        cost_estimate=pl.CostEstimate(flops=30_000_000_000, bytes_accessed=20_000_000, transcendentals=0),
    )(*args)


def mlp_kernel(first, layer, chunks, *refs):
    if first:
        (o_in, xp, xr, gain, next_gain, wo, wg, wu, wd, x_out, h_out, wo_v, wg_v, wu_v, wd_v, o_v, x_v, u_v, si_v, ri_v, load, wl, gs, gr, is_, ir) = refs
    else:
        (o_in, x_in, gain, next_gain, wo, wg, wu, wd, h_out, wo_v, wg_v, wu_v, wd_v, o_v, x_v, u_v, si_v, ri_v, load, wl, gs, gr, is_, ir) = refs
    me = lax.axis_index('model')
    dim = x_v.shape[-1]
    ffn = wg_v.shape[-1]
    rows = chunks * ROWS
    gather = Gather(u_v, gs, gr, me)
    start = [pltpu.make_async_copy(o_in, o_v, load.at[0])]
    start += [pltpu.make_async_copy(wo, wo_v, wl.at[0])]
    if first:
        start += [pltpu.make_async_copy(xp.at[ds(me * ROWS, ROWS)], x_v.at[0], load.at[1])]
        start += [pltpu.make_async_copy(xr.at[0, ds((c - 1) * 256 + me * ROWS, ROWS)], x_v.at[c], load.at[1 + c]) for c in range(1, chunks)]
    else:
        start += [pltpu.make_async_copy(x_in.at[pl.ds(1, chunks)], x_v, load.at[1])]
    weights = [pltpu.make_async_copy(wg.at[layer], wg_v, wl.at[1]), pltpu.make_async_copy(wu.at[layer], wu_v, wl.at[2])]
    downs = [pltpu.make_async_copy(wd.at[lax.rem(me + k, 4)], wd_v.at[k], wl.at[3 + k]) for k in range(4)]
    for cp in start + weights + downs:
        cp.start()
    entry_barrier([('model', lax.rem(me + k, 4)) for k in (1, 2, 3)])
    for cp in start:
        cp.wait()

    def outproj(n, carry):
        cols = ds(n * 256, 256)
        y = dot(o_v[...].reshape(rows, dim), wo_v[:, cols])
        x_v[:, :, cols] = (x_v[:, :, cols].reshape(rows, 256).astype(F32) + y).astype(BF).reshape(chunks, ROWS, 256)
        return carry

    lax.fori_loop(0, dim // 256, outproj, 0)

    for c in range(chunks):
        norm_rows(lambda cols, c=c: x_v[c, :, cols], lambda cols, val, c=c: u_v.__setitem__((c, me, slice(None), cols), val), gain, ROWS, dim)
        if c < 2:
            gather.start(c)
    for cp in weights:
        cp.wait()

    def i_send(c, k):
        return remote(si_v.at[c, lax.rem(me + k, 4)], ri_v.at[3 - k, c], is_.at[k - 1, c], ir.at[k - 1, c], 'model', lax.rem(me + k, 4))

    def i_recv(c, q):
        ref = ri_v.at[q - 1, c]
        return remote(ref, ref, is_.at[3 - q, c], ir.at[3 - q, c], 'model', lax.rem(me + q, 4))

    full = ffn // 256

    def gate_up(c):
        def tile(cols, size):
            lhs = u_v[c].reshape(4 * ROWS, dim)
            g = dot(lhs, wg_v[:, cols])
            p = dot(lhs, wu_v[:, cols])
            si_v[c, :, :, cols] = (g * jax.nn.sigmoid(g) * p).astype(BF).reshape(4, ROWS, size)

        def body(n, carry):
            tile(ds(n * 256, 256), 256)
            return carry

        lax.fori_loop(0, full, body, 0)
        if ffn % 256:
            tile(pl.ds(full * 256, ffn % 256), ffn % 256)

    def down(lo, hi):
        size = hi - lo

        def body(n, carry):
            cols = ds(n * 256, 256)
            y = dot(si_v[lo:hi, me].reshape(size * ROWS, ffn), wd_v[0, :, cols])
            for q in (1, 2, 3):
                y = y + dot(ri_v[q - 1, lo:hi].reshape(size * ROWS, ffn), wd_v[q, :, cols])
            x_v[lo:hi, :, cols] = (x_v[lo:hi, :, cols].reshape(size * ROWS, 256).astype(F32) + y).astype(BF).reshape(size, ROWS, 256)
            return carry

        lax.fori_loop(0, dim // 256, body, 0)
        for c in range(lo, hi):
            norm_rows(lambda cols, c=c: x_v[c, :, cols], lambda cols, val, c=c: o_v.__setitem__((c, slice(None), cols), val), next_gain, ROWS, dim)

    for c in range(chunks + 1):
        if c < chunks:
            gather.forward(c)
            if c + 2 < chunks:
                gather.start(c + 2)
        if c > 0:
            gather.finish(c - 1)
            gate_up(c - 1)
            for k in (2, 1, 3):
                i_send(c - 1, k).start()
    for cp in downs:
        cp.wait()
    split = (chunks + 1) // 2
    outs = []
    for part, (lo, hi) in enumerate(((0, split), (split, chunks))):
        for c in range(lo, hi):
            for q in (1, 2, 3):
                i_recv(c, q).wait_recv()
        down(lo, hi)
        outs.append(pltpu.make_async_copy(o_v.at[pl.ds(lo, hi - lo)], h_out.at[pl.ds(lo, hi - lo)], load.at[part]))
        if first:
            outs.append(pltpu.make_async_copy(x_v.at[pl.ds(lo, hi - lo)], x_out.at[pl.ds(lo, hi - lo)], load.at[2 + part]))
        for cp in outs[-2 if first else -1:]:
            cp.start()
    for cp in outs:
        cp.wait()
    for c in range(chunks):
        gather.drain(c)
        for k in (1, 2, 3):
            i_send(c, k).wait_send()


def mlp(first, layer, collective, o_in, rows_in, gain, next_gain, wo, wg, wu, wd):
    chunks, _, dim = o_in.shape
    ffn = wg.shape[-1]
    args = (o_in, *rows_in, gain, next_gain, wo, wg, wu, wd)
    specs = [ANY] * (1 + len(rows_in)) + [VM, VM] + [ANY] * 4
    out = jax.ShapeDtypeStruct((chunks, ROWS, dim), BF)
    return pl.pallas_call(
        functools.partial(mlp_kernel, first, layer, chunks),
        name=f'mlp{collective}',
        out_shape=(out, out) if first else out,
        in_specs=specs,
        out_specs=(ANY, ANY) if first else ANY,
        scratch_shapes=[
            pltpu.VMEM((dim, dim), BF),
            pltpu.VMEM((dim, ffn), BF),
            pltpu.VMEM((dim, ffn), BF),
            pltpu.VMEM((4, ffn, dim), BF),
            pltpu.VMEM((chunks, ROWS, dim), BF),
            pltpu.VMEM((chunks, ROWS, dim), BF),
            pltpu.VMEM((chunks, 4, ROWS, dim), BF),
            pltpu.VMEM((chunks, 4, ROWS, ffn), BF),
            pltpu.VMEM((3, chunks, ROWS, ffn), BF),
            pltpu.SemaphoreType.DMA((6,)),
            pltpu.SemaphoreType.DMA((7,)),
            pltpu.SemaphoreType.DMA((4, chunks)),
            pltpu.SemaphoreType.DMA((4, chunks)),
            pltpu.SemaphoreType.DMA((3, chunks)),
            pltpu.SemaphoreType.DMA((3, chunks)),
        ],
        compiler_params=pltpu.CompilerParams(collective_id=collective, has_side_effects=True, vmem_limit_bytes=VMEM_BYTES),
        cost_estimate=pl.CostEstimate(flops=80_000_000_000, bytes_accessed=50_000_000, transcendentals=0),
    )(*args)


def head_kernel(chunks, tiles, h_in, wv, target, lens, out, wv_v, u_v, m_v, l_v, p_v, st_v, load, wl, gs, gr, ss, sr):
    me = lax.axis_index('model')
    dim = u_v.shape[-1]
    vocab = wv_v.shape[-1]
    gather = Gather(u_v, gs, gr, me)
    rows = [pltpu.make_async_copy(h_in.at[c], u_v.at[c, me], load.at[c]) for c in range(chunks)]
    span = vocab // tiles
    weights = [pltpu.make_async_copy(wv.at[:, pl.ds(n * span, span)], wv_v.at[:, pl.ds(n * span, span)], wl.at[n]) for n in range(tiles)]
    for cp in rows + weights:
        cp.start()
    entry_barrier([('model', lax.rem(me + k, 4)) for k in (1, 2, 3)])
    for c in range(2):
        rows[c].wait()
        gather.start(c)
    lane = lax.broadcasted_iota(jnp.int32, (256, 128), 1)

    def logits(c, n):
        cols = ds(n * 512, 512)
        s = dot(u_v[c].reshape(256, dim), wv_v[:, cols])
        parts = [s[:, i * 128:(i + 1) * 128] for i in range(4)]
        m = m_v[...]
        top = jnp.maximum(jnp.maximum(parts[0], parts[1]), jnp.maximum(parts[2], parts[3]))
        m_new = jnp.maximum(m, top)
        total = l_v[...] * jnp.exp2((m - m_new) * LOG2E)
        picked = p_v[...]
        wanted = target[pl.ds(c * 256, 256), :] - me * vocab - n * 512
        for i in range(4):
            total = total + jnp.exp2((parts[i] - m_new) * LOG2E)
            picked = picked + jnp.where(wanted - i * 128 == lane, parts[i], 0.0)
        m_v[...] = m_new
        l_v[...] = total
        p_v[...] = picked

    def vocab_pass(c):
        m_v[...] = jnp.full_like(m_v, -jnp.inf)
        l_v[...] = jnp.zeros_like(l_v)
        p_v[...] = jnp.zeros_like(p_v)
        per = span // 512
        if c == 0:
            for t in range(tiles):
                weights[t].wait()
                lax.fori_loop(t * per, (t + 1) * per, lambda n, carry: (logits(c, n), carry)[1], 0)
        else:
            lax.fori_loop(0, vocab // 512, lambda n, carry: (logits(c, n), carry)[1], 0)
        m = m_v[...]
        top = jnp.max(m, axis=-1, keepdims=True)
        total = jnp.sum(l_v[...] * jnp.exp2((m - top) * LOG2E), axis=-1, keepdims=True)
        picked = jnp.sum(p_v[...], axis=-1, keepdims=True)
        stat = jnp.where(lane == 0, top, jnp.where(lane == 1, total, picked))
        st_v[me, :, pl.ds(c * 256, 256)] = stat.T[:8]

    for c in range(chunks + 1):
        if c < chunks:
            gather.forward(c)
            if c + 2 < chunks:
                rows[c + 2].wait()
                gather.start(c + 2)
        if c > 0:
            gather.finish(c - 1)
            vocab_pass(c - 1)

    def st_copy(k, block):
        return remote(st_v.at[block], st_v.at[block], ss.at[k - 1], sr.at[k - 1], 'model', lax.rem(me + k, 4))

    for k in (2, 1, 3):
        st_copy(k, me).start()
    for k in (1, 2, 3):
        st_copy(k, lax.rem(me + 4 - k, 4)).wait_recv()
    tops = [st_v[s, 0:1, :] for s in range(4)]
    top = jnp.maximum(jnp.maximum(tops[0], tops[1]), jnp.maximum(tops[2], tops[3]))
    total = jnp.zeros_like(top)
    picked = jnp.zeros_like(top)
    for s in range(4):
        total = total + st_v[s, 1:2, :] * jnp.exp2((tops[s] - top) * LOG2E)
        picked = picked + st_v[s, 2:3, :]
    value = picked - top - jnp.log(total)
    token = lax.broadcasted_iota(jnp.int32, value.shape, 1)
    out[...] = jnp.where(token < lens[0], value, 0.0)
    for k in (1, 2, 3):
        st_copy(k, me).wait_send()
    for c in range(chunks):
        gather.drain(c)


def head(collective, h_in, wv, target, lens):
    chunks, _, dim = h_in.shape
    vocab = wv.shape[-1]
    tiles = 4
    return pl.pallas_call(
        functools.partial(head_kernel, chunks, tiles),
        name=f'head{collective}',
        out_shape=jax.ShapeDtypeStruct((1, chunks * 256), F32),
        in_specs=[ANY, ANY, VM, pl.BlockSpec(memory_space=pltpu.SMEM)],
        out_specs=VM,
        scratch_shapes=[
            pltpu.VMEM((dim, vocab), BF),
            pltpu.VMEM((chunks, 4, ROWS, dim), BF),
            pltpu.VMEM((256, 128), F32),
            pltpu.VMEM((256, 128), F32),
            pltpu.VMEM((256, 128), F32),
            pltpu.VMEM((4, 8, chunks * 256), F32),
            pltpu.SemaphoreType.DMA((chunks,)),
            pltpu.SemaphoreType.DMA((tiles,)),
            pltpu.SemaphoreType.DMA((4, chunks)),
            pltpu.SemaphoreType.DMA((4, chunks)),
            pltpu.SemaphoreType.DMA((3,)),
            pltpu.SemaphoreType.DMA((3,)),
        ],
        compiler_params=pltpu.CompilerParams(collective_id=collective, has_side_effects=True, vmem_limit_bytes=VMEM_BYTES),
        cost_estimate=pl.CostEstimate(flops=40_000_000_000, bytes_accessed=50_000_000, transcendentals=0),
    )(h_in, wv, target, lens)


def rope_tables(prompt_rows, resp_len, groups):
    half = 64
    freq = ROPE_BASE ** (-jnp.arange(half, dtype=F32) / half)
    pos = jnp.concatenate([lax.axis_index('resp') * prompt_rows + jnp.arange(prompt_rows), prompt_rows * groups + jnp.arange(resp_len)])
    angles = pos.astype(F32)[:, None] * freq
    c, s = jnp.cos(angles), jnp.sin(angles)
    return jnp.concatenate([c, c], axis=-1), jnp.concatenate([-s, s], axis=-1)


def whole(w):
    piece = w.shape[0] // 8
    part = lax.dynamic_slice_in_dim(w, lax.axis_index('resp') * piece, piece, 0)
    return lax.all_gather(part, ('model', 'resp'), axis=0, tiled=True)


def solution(mesh):
    groups = mesh.shape['resp']
    row_axes = ('prompts', 'resp')
    head_spec = P(None, None, 'model', None)
    in_specs = (P(row_axes, None), P(row_axes, None, None), P(row_axes, None), P(row_axes), P(None, None), head_spec, head_spec, head_spec, P(None, 'model', None, None), P(None, None), P(None, None, 'model'), P(None, None, 'model'), P(None, 'model', None), P(None), P(None, 'model'))

    def device_step(x_prompt, x_resp, targets, resp_lens, attn_gain, w_query, w_key, w_value, w_out, mlp_gain, w_gate, w_up, w_down, final_gain, w_vocab):
        dim = x_prompt.shape[-1]
        resp_len = x_resp.shape[1]
        width = w_query.shape[2] * w_query.shape[3]
        layers = w_query.shape[0]
        cos, sin = rope_tables(x_prompt.shape[0], resp_len, groups)
        flat = [[w[l].reshape(dim, width) for w in (w_query, w_key, w_value)] for l in range(layers)]
        outs = [whole(w_out[l].reshape(width, dim)) for l in range(layers)]
        downs = [whole(w_down[l]).reshape(4, w_down.shape[1], dim) for l in range(layers)]
        target = jnp.broadcast_to(targets[0][:, None], (resp_len, 128))
        o = attention(True, 0, (x_prompt, x_resp), attn_gain[0:1], *flat[0], cos, sin)
        x, h = mlp(True, 0, 1, o, (x_prompt, x_resp), mlp_gain[0:1], attn_gain[1:2], outs[0], w_gate, w_up, downs[0])
        o = attention(False, 2, (h,), None, *flat[1], cos, sin)
        h = mlp(False, 1, 3, o, (x,), mlp_gain[1:2], final_gain[None, :], outs[1], w_gate, w_up, downs[1])
        return head(4, h, w_vocab, target, resp_lens)

    return jax.shard_map(device_step, mesh=mesh, in_specs=in_specs, out_specs=P(row_axes, None), check_vma=False)
```

```python
import functools

import jax
import jax.numpy as jnp
from jax import lax
from jax.experimental import pallas as pl
from jax.experimental.pallas import tpu as pltpu
from jax.sharding import PartitionSpec as P

EPS = 1e-6
ROPE_BASE = 10000.0
LOG2E = 1.4426950408889634
VMEM_BYTES = 67043328
ROWS = 64
LANES = 128
BLOCK = 256
BF = jnp.bfloat16
F32 = jnp.float32
ANY = pl.BlockSpec(memory_space=pl.ANY)
VM = pl.BlockSpec(memory_space=pltpu.VMEM)
MESH = pl.DeviceIdType.MESH
RIGHT, LEFT, RIGHT_ON, LEFT_ON, OWN_MATE, LEFT_MATE, RIGHT_MATE, OPP_MATE = range(8)


def ds(index, size):
    return pl.ds(pl.multiple_of(index * size, size), size)


def dot(a, b):
    return jnp.dot(a, b, preferred_element_type=F32)


def dot_t(a, b):
    return lax.dot_general(a, b, (((1,), (1,)), ((), ())), preferred_element_type=F32)


def sems(*shape):
    return pltpu.SemaphoreType.DMA(shape)


def remote(src, dst, send, recv, axis, where):
    return pltpu.make_async_remote_copy(src_ref=src, dst_ref=dst, send_sem=send, recv_sem=recv, device_id={axis: where}, device_id_type=MESH)


def local(src, dst, sem):
    copy = pltpu.make_async_copy(src, dst, sem)
    copy.start()
    return copy


def greet(rings):
    barrier = pltpu.get_barrier_semaphore()
    peers = {}
    for ring in rings:
        for i, where in enumerate(ring.places[1:]):
            peers[ring.axis, i] = (ring.axis, where)
        if ring.mate is not None:
            peers['mate'] = (ring.axis, ring.mate)
    for axis, where in peers.values():
        pl.semaphore_signal(barrier, inc=1, device_id={axis: where}, device_id_type=MESH)
    pl.semaphore_wait(barrier, len(peers))


class Ring:
    def __init__(self, axis, me, stride, piece, send, recv, source=None, mate=None):
        self.axis, self.piece, self.send, self.recv, self.source, self.mate = axis, piece, send, recv, source, mate
        self.places = [lax.rem(me + k * stride, 4 * stride) for k in range(4)]
        self.own, self.right, self.opp, self.left = self.places
        self.mate_step = None if mate is None else mate - me

    def copy(self, kind, u, owner, source=None):
        dst = self.piece(u, owner)
        if kind in (RIGHT_ON, LEFT_ON):
            half = dst.shape[0] // 2
            dst = dst.at[pl.ds((kind - RIGHT_ON) * half, half)]
        where = self.mate if kind >= OWN_MATE else self.left if kind in (LEFT, LEFT_ON) else self.right
        return remote(dst if source is None else source, dst, self.send.at[kind, u], self.recv.at[kind, u], self.axis, where)

    def start(self, u):
        for kind in (OWN_MATE, RIGHT, LEFT)[self.mate is None:]:
            self.copy(kind, u, self.own, self.source and self.source(u)).start()

    def forward(self, u):
        for kind, owner in ((RIGHT, self.left), (LEFT, self.right)):
            self.copy(kind, u, owner).wait_recv()
            self.copy(kind + RIGHT_ON, u, owner).start()
            if self.mate is not None:
                self.copy(kind + LEFT_MATE, u, owner).start()

    def finish(self, u):
        for kind in (RIGHT_ON, LEFT_ON):
            self.copy(kind, u, self.opp).wait_recv()
        if self.mate is not None:
            self.copy(OPP_MATE, u, self.opp).start()

    def mate_arrived(self, u):
        for kind, owner in ((OWN_MATE, self.own), (LEFT_MATE, self.left), (RIGHT_MATE, self.right), (OPP_MATE, self.opp)):
            self.copy(kind, u, owner + self.mate_step).wait_recv()

    def drain(self, u):
        for kind, owner in ((RIGHT, self.own), (LEFT, self.own), (RIGHT_ON, self.left), (LEFT_ON, self.right), (OWN_MATE, self.own), (LEFT_MATE, self.left), (RIGHT_MATE, self.right), (OPP_MATE, self.opp)):
            if kind < OWN_MATE or self.mate is not None:
                self.copy(kind, u, owner).wait_send()


def resp_ring(piece, send, recv, source=None):
    r = lax.axis_index('resp')
    return Ring('resp', r, 2, piece, send, recv, source, r + 1 - 2 * lax.rem(r, 2))


def model_ring(piece, send, recv, source=None):
    return Ring('model', lax.axis_index('model'), 1, piece, send, recv, source)


def norm_rows(src, dst, gain_ref, rows, width):
    def square(n, total):
        block = src(ds(n, BLOCK)).astype(F32)
        sq = block * block
        return total + sq[:, :LANES] + sq[:, LANES:]

    trips = width // BLOCK
    total = lax.fori_loop(0, trips, square, jnp.zeros((rows, LANES), F32), unroll=2)
    inv = lax.rsqrt(jnp.sum(total, axis=-1, keepdims=True) / width + EPS)

    def scale(n, carry):
        cols = ds(n, BLOCK)
        dst(cols, (src(cols).astype(F32) * inv * gain_ref[:, cols]).astype(BF))
        return carry

    lax.fori_loop(0, trips, scale, 0, unroll=2)


def loop(lo, hi, body):
    def wrapped(i, carry):
        body(i)
        return carry
    lax.fori_loop(lo, hi, wrapped, 0)


def when(condition, *actions):
    @pl.when(condition)
    def _():
        for action in actions:
            action()


def params(collective):
    return pltpu.CompilerParams(collective_id=collective, has_side_effects=True, vmem_limit_bytes=VMEM_BYTES)


def work(flops):
    return pl.CostEstimate(flops=flops, bytes_accessed=flops // 1000, transcendentals=0)


def attention_kernel(first, layer, chunks, *refs):
    if first:
        xp, xr, gain, *refs = refs
    else:
        hin, *refs = refs
    wq, wk, wv, cos, sin, w_out, w_down, o_out, wo_all, wo_y, wd_y, *refs = refs
    if first:
        x_v, *refs = refs
    h_v, q_v, k_v, v_v, acc_v, m_v, l_v, o_v, load, h_s, h_r, kv_s, kv_r, y_s, y_r, wo_s, wo_r, o_s, o_r, own_s = refs
    me, r = lax.axis_index('model'), lax.axis_index('resp')
    chip = r // 2
    width = wq.shape[-1]
    dim = wq.shape[0]
    heads = width // LANES
    log_scale = LOG2E * LANES ** -0.5
    prompt_blocks = k_v.shape[0] - (chunks - 1)

    gather = model_ring(lambda c, b: h_v.at[c, b], h_s, h_r)
    kv = resp_ring(lambda u, b: (k_v, v_v)[u].at[b], kv_s, kv_r)
    ours = ds(r, BLOCK)
    spread = model_ring(lambda u, b: (wo_y, wd_y)[u].at[b], y_s, y_r, lambda u: (w_out, w_down)[u].at[layer, :, ours])
    shares = spread.places[1:]
    outs = resp_ring(lambda u, b: wo_all.at[shares[u], :, ds(b, BLOCK)], wo_s, wo_r, lambda u: wo_y.at[shares[u]])

    if first:
        loads = [local(xp, x_v.at[0], load.at[0])] + [local(xr.at[0, pl.ds((c - 1) * BLOCK, BLOCK)], x_v.at[c], load.at[c]) for c in range(1, chunks)]
    else:
        loads = [local(hin.at[c], h_v.at[c, me], load.at[c]) for c in range(chunks)]
    greet([gather, kv])
    own_cols = []

    def spread_done(u):
        spread.finish(u)
        if u == 0:
            for s in range(3):
                outs.start(s)
                own_cols.append(local(wo_y.at[shares[s]], wo_all.at[shares[s], :, ours], own_s.at[s]))

    def key_block(c):
        return jnp.where(c == 0, r, prompt_blocks + c - 1)

    def project(c):
        rows = pl.ds(pl.multiple_of(c * BLOCK, BLOCK), BLOCK)
        cs, sn = cos[rows, :], sin[rows, :]
        blk = key_block(c)
        for which, w in enumerate((wk, wv, wq)):
            for n in range(width // BLOCK):
                y = dot(h_v[c].reshape(BLOCK, dim), w[:, pl.ds(n * BLOCK, BLOCK)])
                for i in range(2):
                    cols = pl.ds((2 * n + i) * LANES, LANES)
                    part = y[:, i * LANES:(i + 1) * LANES]
                    if which == 1:
                        v_v[blk, cols, :] = part.T.astype(BF)
                    else:
                        part = (part * cs + pltpu.roll(part, LANES // 2, 1) * sn).astype(BF)
                        if which == 2:
                            q_v[c, :, cols] = part
                        else:
                            k_v[blk, :, cols] = part

    kv_units = range(2)

    def kv_do(name):
        for u in kv_units:
            getattr(kv, name)(u)

    if first:
        spread.start(0)
        spread.start(1)

        def chunk(c):
            norm_rows(lambda cols: x_v[c, :, cols], lambda cols, val: h_v.__setitem__((c, slice(None), slice(None), cols), val.reshape(4, ROWS, BLOCK)), gain, BLOCK, dim)
            project(c)
            when(c == 0, lambda: kv_do('start'))
            when(c == 2, lambda: spread.forward(0))

        for cp in loads:
            cp.wait()
        loop(0, chunks, chunk)
    else:
        for c in range(2):
            loads[c].wait()
            gather.start(c)
        for cp in loads[2:]:
            cp.wait()

        def chunk(c):
            def receive():
                gather.forward(c)
                when(c + 2 < chunks, lambda: gather.start(c + 2))
            when(c < chunks, receive)

            def use():
                gather.finish(c - 1)
                project(c - 1)
            when(c > 0, use)
            when(c == 1, lambda: kv_do('start'))
            when(c == chunks - 1, lambda: kv_do('forward'))

        loop(0, chunks + 1, chunk)
        spread.start(0)
        spread.start(1)

    key_i = lax.broadcasted_iota(jnp.int32, (BLOCK, BLOCK), 0)
    causal = key_i <= lax.broadcasted_iota(jnp.int32, (BLOCK, BLOCK), 1)

    def step(qi, kb, blocks, diagonal=False):
        def scores(n):
            cols = pl.ds(n * LANES, LANES)
            s = dot_t(k_v[pl.ds(kb, blocks), :, cols].reshape(blocks * BLOCK, LANES), q_v[qi, :, cols])
            return jnp.where(causal, s, -jnp.inf) if diagonal else s

        ahead = scores(0)
        for n in range(heads):
            s = ahead
            if n + 1 < heads:
                ahead = scores(n + 1)
            top = jnp.max(s, axis=0, keepdims=True)
            if not diagonal:
                m = m_v[qi, n, :1]
                top = jnp.maximum(m, top)
            p = jnp.exp2((s - top) * log_scale)
            total = jnp.sum(p, axis=0, keepdims=True)
            p = p.astype(BF)
            mixed = None
            for b in range(blocks):
                part = dot(v_v[kb + b, pl.ds(n * LANES, LANES), :], p[b * BLOCK:(b + 1) * BLOCK])
                mixed = part if mixed is None else mixed + part
            if not diagonal:
                alpha = jnp.exp2((m - top) * log_scale)
                total = total + l_v[qi, n, :1] * alpha
                mixed = mixed + acc_v[qi, n] * alpha
            m_v[qi, n, :1] = top
            l_v[qi, n, :1] = total
            acc_v[qi, n] = mixed

    low = 0 if first else 1

    def own(qi):
        step(qi, key_block(qi), 1, True)
        loop(prompt_blocks, prompt_blocks + qi - 1, lambda b: step(qi, b, 1))

    loop(low, chunks, own)

    if first:
        spread_done(0)
        kv_do('forward')
        spread.forward(1)
    kv_do('finish')
    kv_do('mate_arrived')
    if not first:
        spread.forward(0)

    def o_copy(c, k):
        owner = spread.places[k]
        return remote(o_v.at[c, owner], o_out.at[c, :, ds(me, width)], o_s.at[k - 1, c], o_r.at[k - 1, c], 'model', owner)

    def o_own(c):
        return pltpu.make_async_copy(o_v.at[c, me], o_out.at[c, :, ds(me, width)], load.at[c])

    def prompt(qi):
        c = qi - low
        loop(0, jnp.where(qi == 0, chip, 4), lambda x: step(qi, 2 * x, 2))
        when((qi == 0) & (r > 2 * chip), lambda: step(qi, 2 * chip, 1))
        for n in range(heads):
            out = (acc_v[qi, n] / l_v[qi, n, :1]).T.astype(BF)
            o_v[c, :, :, pl.ds(n * LANES, LANES)] = out.reshape(4, ROWS, LANES)
        for k in (2, 1, 3):
            o_copy(c, k).start()
        o_own(c).start()

    events = [lambda: outs.forward(0), lambda: outs.forward(1), lambda: (outs.forward(2), outs.finish(0)), lambda: outs.finish(1)]
    if not first:
        events = []

    def prompt_and_events(qi):
        prompt(qi)
        for i, event in enumerate(events):
            when(qi == i + low, event)

    loop(low, chunks, prompt_and_events)
    if first:
        spread_done(1)
        outs.finish(2)
    else:
        spread_done(0)
        spread.forward(1)
        for s in range(3):
            outs.forward(s)
        for s in range(3):
            outs.finish(s)
        spread_done(1)
    for s in range(3):
        outs.mate_arrived(s)
        outs.drain(s)
        own_cols[s].wait()
    for u in kv_units:
        kv.drain(u)
        spread.drain(u)
    for c in range(chunks - low):
        for k in (1, 2, 3):
            o_copy(c, k).wait()
        o_own(c).wait()
    if not first:
        for c in range(chunks):
            gather.drain(c)


def attention(first, layer, collective, hidden, gain, wq, wk, wv, cos, sin, w_out, w_down):
    dim, width = wq.shape
    chunks = cos.shape[0] // BLOCK
    outs = chunks if first else chunks - 1
    heads = width // LANES
    blocks = lax.psum(1, 'resp') + chunks - 1
    args = hidden + ((gain,) if first else ()) + (wq, wk, wv, cos, sin, w_out, w_down)
    specs = [ANY] * len(hidden) + [VM] * (len(args) - len(hidden) - 2) + [ANY] * 2
    ffn = w_down.shape[1]
    shapes = [(outs, ROWS, 4 * width), (4, width, dim), (4, width, BLOCK), (4, ffn, BLOCK)]
    scratch = [pltpu.VMEM((chunks, BLOCK, dim), BF)] if first else []
    state = pltpu.VMEM((chunks, heads, 8, BLOCK), F32)
    scratch += [
        pltpu.VMEM((chunks, 4, ROWS, dim), BF),
        pltpu.VMEM((chunks, BLOCK, width), BF),
        pltpu.VMEM((blocks, BLOCK, width), BF),
        pltpu.VMEM((blocks, width, BLOCK), BF),
        pltpu.VMEM((chunks, heads, LANES, BLOCK), F32),
        state,
        state,
        pltpu.VMEM((outs, 4, ROWS, width), BF),
        sems(chunks),
    ]
    for kinds, units in ((4, chunks), (8, 2), (4, 2), (8, 3), (3, outs)):
        scratch += [sems(kinds, units)] * 2
    scratch.append(sems(3))
    return pl.pallas_call(
        functools.partial(attention_kernel, first, layer, chunks),
        name=f'attention{layer}',
        out_shape=tuple(jax.ShapeDtypeStruct(s, BF) for s in shapes),
        in_specs=specs,
        out_specs=(ANY,) * len(shapes),
        scratch_shapes=scratch,
        compiler_params=params(collective),
        cost_estimate=work(30_000_000_000),
    )(*args)


def mlp_kernel(first, layer, chunks, *refs):
    o_in, *rows_in, gain, next_gain, w_out, wo_all, wg, wu, w_down, wd_y, h_out = refs[:12 if first else 11]
    refs = refs[12 if first else 11:]
    if first:
        x_out, *refs = refs
    wo_v, wg_v, wu_v, wd_v, o_v, x_v, u_v, si_v, ri_v, load, wl, wd_l, h_s, h_r, x_s, x_r, i_s, i_r = refs
    me, r = lax.axis_index('model'), lax.axis_index('resp')
    dim = x_v.shape[-1]
    ffn = wg_v.shape[0]
    width = wo_v.shape[1]
    rows = chunks * ROWS
    gather = model_ring(lambda c, b: u_v.at[c, b], h_s, h_r)
    shares = gather.places[1:]
    downs = resp_ring(lambda u, b: wd_v.at[u + 1, :, ds(b, BLOCK)], x_s, x_r, lambda u: wd_y.at[shares[u]])

    start = [local(o_in, o_v, load.at[0]), local(w_out.at[layer], wo_v.at[me], wl.at[0])]
    start += [local(wo_all.at[s], wo_v.at[s], wl.at[i]) for i, s in enumerate(shares, 1)]
    if first:
        start += [local(rows_in[0].at[ds(me, ROWS)], x_v.at[0], load.at[1])]
        start += [local(rows_in[1].at[0, ds((c - 1) * 4 + me, ROWS)], x_v.at[c], load.at[1 + c]) for c in range(1, chunks)]
    else:
        start += [local(rows_in[0].at[pl.ds(1, chunks)], x_v, load.at[1])]
    weights = [local(wg.at[layer], wg_v, wl.at[4]), local(wu.at[layer], wu_v, wl.at[5])]
    greet([gather, downs])
    for u in range(3):
        downs.start(u)
    kept = [local(w_down.at[layer], wd_v.at[0], wd_l.at[0])]
    kept += [local(wd_y.at[s], wd_v.at[i, :, ds(r, BLOCK)], wd_l.at[i]) for i, s in enumerate(shares, 1)]
    for cp in start:
        cp.wait()

    def outproj(n):
        cols = ds(n, 2 * BLOCK)
        y = dot(o_v[...].reshape(rows, dim), wo_v[:, :, cols].reshape(dim, 2 * BLOCK))
        x_v[:, :, cols] = (x_v[:, :, cols].reshape(rows, 2 * BLOCK).astype(F32) + y).astype(BF).reshape(chunks, ROWS, 2 * BLOCK)

    loop(0, dim // (2 * BLOCK), outproj)

    def normalize(c):
        norm_rows(lambda cols: x_v[c, :, cols], lambda cols, val: u_v.__setitem__((c, me, slice(None), cols), val), gain, ROWS, dim)
        when(c < 2, lambda: gather.start(c))

    loop(0, chunks, normalize)
    for cp in weights:
        cp.wait()

    def i_send(c, k):
        return remote(si_v.at[c, gather.places[k]], ri_v.at[3 - k, c], i_s.at[k - 1, c], i_r.at[k - 1, c], 'model', gather.places[k])

    def i_recv(c, q):
        ref = ri_v.at[q - 1, c]
        return remote(ref, ref, i_s.at[3 - q, c], i_r.at[3 - q, c], 'model', gather.places[q])

    def gate_up(c):
        lhs = u_v[c].reshape(4 * ROWS, dim)
        half = ffn // 2
        for lo in (0, half):
            cols = pl.ds(lo, half)
            g = dot_t(lhs, wg_v[cols, :])
            inner = (g * jax.nn.sigmoid(g) * dot_t(lhs, wu_v[cols, :])).astype(BF)
            si_v[c, :, :, cols] = inner.reshape(4, ROWS, half)
        for k in (2, 1, 3):
            i_send(c, k).start()

    events = {2: lambda: downs.forward(0), 3: lambda: downs.forward(1), 4: lambda: (downs.forward(2), downs.finish(0))}

    def chunk(c):
        def receive():
            gather.forward(c)
            when(c + 2 < chunks, lambda: gather.start(c + 2))
        when(c < chunks, receive)

        def use():
            gather.finish(c - 1)
            gate_up(c - 1)
        when(c > 0, use)
        for at, event in events.items():
            when(c == at, event)

    loop(0, chunks + 1, chunk)
    downs.finish(1)
    downs.finish(2)
    for u in range(3):
        downs.mate_arrived(u)
    for cp in kept:
        cp.wait()

    def down(lo, hi):
        size = hi - lo

        def tile(n):
            cols = ds(n, BLOCK)
            y = dot(si_v[lo:hi, me].reshape(size * ROWS, ffn), wd_v[0, :, cols])
            for q in (1, 2, 3):
                y = y + dot(ri_v[q - 1, lo:hi].reshape(size * ROWS, ffn), wd_v[q, :, cols])
            x_v[lo:hi, :, cols] = (x_v[lo:hi, :, cols].reshape(size * ROWS, BLOCK).astype(F32) + y).astype(BF).reshape(size, ROWS, BLOCK)

        loop(0, dim // BLOCK, tile)
        loop(lo, hi, lambda c: norm_rows(lambda cols: x_v[c, :, cols], lambda cols, val: o_v.__setitem__((c, slice(None), cols), val), next_gain, ROWS, dim))

    split = (chunks + 1) // 2
    stored = []
    for part, (lo, hi) in enumerate(((0, split), (split, chunks))):
        for c in range(lo, hi):
            for q in (1, 2, 3):
                i_recv(c, q).wait_recv()
        down(lo, hi)
        span = pl.ds(lo, hi - lo)
        stored.append(local(o_v.at[span], h_out.at[span], load.at[part]))
        if first:
            stored.append(local(x_v.at[span], x_out.at[span], load.at[2 + part]))
    for cp in stored:
        cp.wait()
    for u in range(3):
        downs.drain(u)
    for c in range(chunks):
        gather.drain(c)
        for k in (1, 2, 3):
            i_send(c, k).wait_send()


def mlp(first, layer, collective, o_in, rows_in, gain, next_gain, w_out, wo_all, wg, wu, w_down, wd_y):
    chunks, _, dim = o_in.shape
    ffn = wg.shape[1]
    args = (o_in, *rows_in, gain, next_gain, w_out, wo_all, wg, wu, w_down, wd_y)
    specs = [ANY] * (1 + len(rows_in)) + [VM] * 2 + [ANY] * 6
    count = 2 if first else 1
    scratch = [pltpu.VMEM(s, BF) for s in (wo_all.shape, (ffn, dim), (ffn, dim), (4, ffn, dim), (chunks, ROWS, dim), (chunks, ROWS, dim), (chunks, 4, ROWS, dim), (chunks, 4, ROWS, ffn), (3, chunks, ROWS, ffn))]
    scratch += [sems(6), sems(6), sems(4)]
    for kinds, units in ((4, chunks), (8, 3), (3, chunks)):
        scratch += [sems(kinds, units)] * 2
    return pl.pallas_call(
        functools.partial(mlp_kernel, first, layer, chunks),
        name=f'mlp{layer}',
        out_shape=(jax.ShapeDtypeStruct((chunks, ROWS, dim), BF),) * count,
        in_specs=specs,
        out_specs=(ANY,) * count,
        scratch_shapes=scratch,
        compiler_params=params(collective),
        cost_estimate=work(80_000_000_000),
    )(*args)


def head_kernel(chunks, tiles, h_in, wv, target, lens, out, wv_v, u_v, m_v, l_v, p_v, st_v, load, wl, h_s, h_r, st_s, st_r):
    me = lax.axis_index('model')
    dim, vocab = wv_v.shape
    span = vocab // tiles
    tile = 4 * BLOCK
    gather = model_ring(lambda c, b: u_v.at[c, b], h_s, h_r)
    rows = [local(h_in.at[c], u_v.at[c, me], load.at[c]) for c in range(chunks)]

    def weight(t):
        cols = ds(t, span)
        return pltpu.make_async_copy(wv.at[:, cols], wv_v.at[:, cols], wl.at[t])

    loop(0, tiles, lambda t: weight(t).start())
    greet([gather])
    for cp in rows:
        cp.wait()
    for c in range(2):
        gather.start(c)
    lane = lax.broadcasted_iota(jnp.int32, (BLOCK, LANES), 1)
    pieces = range(tile // LANES)

    def logits(c, n):
        s = dot(u_v[c].reshape(BLOCK, dim), wv_v[:, ds(n, tile)])
        parts = [s[:, i * LANES:(i + 1) * LANES] for i in pieces]
        m = m_v[...]
        top = functools.reduce(jnp.maximum, parts, m)
        total = l_v[...] * jnp.exp2((m - top) * LOG2E)
        picked = p_v[...]
        wanted = target[ds(c, BLOCK), :] - me * vocab - n * tile
        for i in pieces:
            total = total + jnp.exp2((parts[i] - top) * LOG2E)
            picked = picked + jnp.where(wanted - i * LANES == lane, parts[i], 0.0)
        m_v[...] = top
        l_v[...] = total
        p_v[...] = picked

    def vocab_pass(c):
        m_v[...] = jnp.full_like(m_v, -jnp.inf)
        l_v[...] = jnp.zeros_like(l_v)
        p_v[...] = jnp.zeros_like(p_v)
        per = span // tile

        def columns(n):
            when((c == 0) & (lax.rem(n, per) == 0), lambda: weight(n // per).wait())
            logits(c, n)

        loop(0, vocab // tile, columns)
        m = m_v[...]
        top = jnp.max(m, axis=-1, keepdims=True)
        total = jnp.sum(l_v[...] * jnp.exp2((m - top) * LOG2E), axis=-1, keepdims=True)
        picked = jnp.sum(p_v[...], axis=-1, keepdims=True)
        stat = jnp.where(lane == 0, top, jnp.where(lane == 1, total, picked))
        st_v[me, :, ds(c, BLOCK)] = stat.T[:8]

    def chunk(c):
        def receive():
            gather.forward(c)
            when(c + 2 < chunks, lambda: gather.start(c + 2))
        when(c < chunks, receive)

        def use():
            gather.finish(c - 1)
            vocab_pass(c - 1)
        when(c > 0, use)

    loop(0, chunks + 1, chunk)

    def st_copy(k, block):
        return remote(st_v.at[block], st_v.at[block], st_s.at[k - 1], st_r.at[k - 1], 'model', gather.places[k])

    for k in (2, 1, 3):
        st_copy(k, me).start()
    for k in (1, 2, 3):
        st_copy(k, gather.places[4 - k]).wait_recv()
    tops = [st_v[s, 0:1, :] for s in range(4)]
    top = functools.reduce(jnp.maximum, tops)
    total = sum(st_v[s, 1:2, :] * jnp.exp2((tops[s] - top) * LOG2E) for s in range(4))
    value = sum(st_v[s, 2:3, :] for s in range(4)) - top - jnp.log(total)
    token = lax.broadcasted_iota(jnp.int32, value.shape, 1)
    out[...] = jnp.where(token < lens[0], value, 0.0)
    for k in (1, 2, 3):
        st_copy(k, me).wait_send()
    for c in range(chunks):
        gather.drain(c)


def head(collective, h_in, wv, target, lens):
    chunks, _, dim = h_in.shape
    tiles = 4
    stat = pltpu.VMEM((BLOCK, LANES), F32)
    return pl.pallas_call(
        functools.partial(head_kernel, chunks, tiles),
        name='head',
        out_shape=jax.ShapeDtypeStruct((1, chunks * BLOCK), F32),
        in_specs=[ANY, ANY, VM, pl.BlockSpec(memory_space=pltpu.SMEM)],
        out_specs=VM,
        scratch_shapes=[
            pltpu.VMEM(wv.shape, BF),
            pltpu.VMEM((chunks, 4, ROWS, dim), BF),
            stat,
            stat,
            stat,
            pltpu.VMEM((4, 8, chunks * BLOCK), F32),
            sems(chunks),
            sems(tiles),
        ] + [sems(4, chunks)] * 2 + [sems(3)] * 2,
        compiler_params=params(collective),
        cost_estimate=work(40_000_000_000),
    )(h_in, wv, target, lens)


def rope_tables(prompt_rows, resp_len, groups):
    half = LANES // 2
    freq = ROPE_BASE ** (-jnp.arange(half, dtype=F32) / half)
    pos = jnp.concatenate([lax.axis_index('resp') * prompt_rows + jnp.arange(prompt_rows), prompt_rows * groups + jnp.arange(resp_len)])
    angles = pos.astype(F32)[:, None] * freq
    c, s = jnp.cos(angles), jnp.sin(angles)
    return jnp.concatenate([c, c], axis=-1), jnp.concatenate([-s, s], axis=-1)


def solution(mesh):
    groups = mesh.shape['resp']
    row_axes = ('prompts', 'resp')
    head_spec = P(None, None, 'model', None)
    in_specs = (P(row_axes, None), P(row_axes, None, None), P(row_axes, None), P(row_axes), P(None, None), head_spec, head_spec, head_spec, P(None, 'model', None, None), P(None, None), P(None, None, 'model'), P(None, None, 'model'), P(None, 'model', None), P(None), P(None, 'model'))

    def device_step(x_prompt, x_resp, targets, resp_lens, attn_gain, w_query, w_key, w_value, w_out, mlp_gain, w_gate, w_up, w_down, final_gain, w_vocab):
        layers, dim, heads, head_dim = w_query.shape
        width = heads * head_dim
        resp_len = x_resp.shape[1]
        cos, sin = rope_tables(x_prompt.shape[0], resp_len, groups)
        flat = [[w[l].reshape(dim, width) for w in (w_query, w_key, w_value)] for l in range(layers)]
        w_out = w_out.reshape(layers, width, dim)
        gates = [jnp.swapaxes(w, 1, 2) for w in (w_gate, w_up)]
        gains = [attn_gain[l:l + 1] for l in range(layers)] + [final_gain[None, :]]
        target = jnp.broadcast_to(targets[0][:, None], (resp_len, LANES))
        rows = (x_prompt, x_resp)
        hidden = rows
        for l in range(layers):
            first = l == 0
            o, wo_all, _, wd_y = attention(first, l, 2 * l, hidden, gains[l], *flat[l], cos, sin, w_out, w_down)
            h, *rows = mlp(first, l, 2 * l + 1, o, rows, mlp_gain[l:l + 1], gains[l + 1], w_out, wo_all, *gates, w_down, wd_y)
            hidden = (h,)
        return head(2 * layers, h, w_vocab, target, resp_lens)

    return jax.shard_map(device_step, mesh=mesh, in_specs=in_specs, out_specs=P(row_axes, None), check_vma=False)
```

```python
import functools

import jax
import jax.numpy as jnp
from jax import lax
from jax.experimental import pallas as pl
from jax.experimental.pallas import tpu as pltpu
from jax.sharding import PartitionSpec as P

EPS = 1e-6
ROPE_BASE = 10000.0
LOG2E = 1.4426950408889634
VMEM_BYTES = 67043328
ROWS = 64
LANES = 128
BLOCK = 256
BF = jnp.bfloat16
F32 = jnp.float32
ANY = pl.BlockSpec(memory_space=pl.ANY)
VM = pl.BlockSpec(memory_space=pltpu.VMEM)
MESH = pl.DeviceIdType.MESH
RIGHT, LEFT, RIGHT_ON, LEFT_ON, OWN_MATE, LEFT_MATE, RIGHT_MATE, OPP_MATE = range(8)


def ds(index, size):
    return pl.ds(pl.multiple_of(index * size, size), size)


def dot(a, b):
    return jnp.dot(a, b, preferred_element_type=F32)


def dot_t(a, b):
    return lax.dot_general(a, b, (((1,), (1,)), ((), ())), preferred_element_type=F32)


def sems(*shape):
    return pltpu.SemaphoreType.DMA(shape)


def remote(src, dst, send, recv, axis, where):
    return pltpu.make_async_remote_copy(src_ref=src, dst_ref=dst, send_sem=send, recv_sem=recv, device_id={axis: where}, device_id_type=MESH)


def local(src, dst, sem):
    copy = pltpu.make_async_copy(src, dst, sem)
    copy.start()
    return copy


def greet(rings):
    barrier = pltpu.get_barrier_semaphore()
    peers = {}
    for ring in rings:
        for i, where in enumerate(ring.places[1:]):
            peers[ring.axis, i] = (ring.axis, where)
        if ring.mate is not None:
            peers['mate'] = (ring.axis, ring.mate)
    for axis, where in peers.values():
        pl.semaphore_signal(barrier, inc=1, device_id={axis: where}, device_id_type=MESH)
    pl.semaphore_wait(barrier, len(peers))


class Ring:
    def __init__(self, axis, me, stride, piece, send, recv, source=None, mate=None):
        self.axis, self.piece, self.send, self.recv, self.source, self.mate = axis, piece, send, recv, source, mate
        self.places = [lax.rem(me + k * stride, 4 * stride) for k in range(4)]
        self.own, self.right, self.opp, self.left = self.places
        self.mate_step = None if mate is None else mate - me

    def copy(self, kind, u, owner, source=None):
        dst = self.piece(u, owner)
        if kind in (RIGHT_ON, LEFT_ON):
            half = dst.shape[0] // 2
            dst = dst.at[pl.ds((kind - RIGHT_ON) * half, half)]
        where = self.mate if kind >= OWN_MATE else self.left if kind in (LEFT, LEFT_ON) else self.right
        return remote(dst if source is None else source, dst, self.send.at[kind, u], self.recv.at[kind, u], self.axis, where)

    def start(self, u):
        for kind in (OWN_MATE, RIGHT, LEFT)[self.mate is None:]:
            self.copy(kind, u, self.own, self.source and self.source(u)).start()

    def forward(self, u):
        for kind, owner in ((RIGHT, self.left), (LEFT, self.right)):
            self.copy(kind, u, owner).wait_recv()
            self.copy(kind + RIGHT_ON, u, owner).start()
            if self.mate is not None:
                self.copy(kind + LEFT_MATE, u, owner).start()

    def finish(self, u):
        for kind in (RIGHT_ON, LEFT_ON):
            self.copy(kind, u, self.opp).wait_recv()
        if self.mate is not None:
            self.copy(OPP_MATE, u, self.opp).start()

    def mate_has(self, u, kind):
        owner = {OWN_MATE: self.own, LEFT_MATE: self.left, RIGHT_MATE: self.right, OPP_MATE: self.opp}[kind]
        self.copy(kind, u, owner + self.mate_step).wait_recv()

    def mate_arrived(self, u):
        for kind in range(OWN_MATE, OPP_MATE + 1):
            self.mate_has(u, kind)

    def drain(self, u):
        for kind, owner in ((RIGHT, self.own), (LEFT, self.own), (RIGHT_ON, self.left), (LEFT_ON, self.right), (OWN_MATE, self.own), (LEFT_MATE, self.left), (RIGHT_MATE, self.right), (OPP_MATE, self.opp)):
            if kind < OWN_MATE or self.mate is not None:
                self.copy(kind, u, owner).wait_send()


def resp_ring(piece, send, recv, source=None):
    r = lax.axis_index('resp')
    return Ring('resp', r, 2, piece, send, recv, source, r + 1 - 2 * lax.rem(r, 2))


def model_ring(piece, send, recv, source=None):
    return Ring('model', lax.axis_index('model'), 1, piece, send, recv, source)


def norm_rows(src, dst, gain_ref, rows, width):
    def square(n, total):
        block = src(ds(n, BLOCK)).astype(F32)
        sq = block * block
        return total + sq[:, :LANES] + sq[:, LANES:]

    trips = width // BLOCK
    total = lax.fori_loop(0, trips, square, jnp.zeros((rows, LANES), F32), unroll=2)
    inv = lax.rsqrt(jnp.sum(total, axis=-1, keepdims=True) / width + EPS)

    def scale(n, carry):
        cols = ds(n, BLOCK)
        dst(cols, (src(cols).astype(F32) * inv * gain_ref[:, cols]).astype(BF))
        return carry

    lax.fori_loop(0, trips, scale, 0, unroll=2)


def loop(lo, hi, body):
    def wrapped(i, carry):
        body(i)
        return carry
    lax.fori_loop(lo, hi, wrapped, 0)


def when(condition, *actions):
    @pl.when(condition)
    def _():
        for action in actions:
            action()


def params(collective):
    return pltpu.CompilerParams(collective_id=collective, has_side_effects=True, vmem_limit_bytes=VMEM_BYTES)


def work(flops):
    return pl.CostEstimate(flops=flops, bytes_accessed=flops // 1000, transcendentals=0)


def attention_kernel(first, layer, chunks, *refs):
    if first:
        xp, xr, gain, *refs = refs
    else:
        h0, hin, *refs = refs
    cos, sin, *refs = refs
    heads_in, (w_out, w_down, o_out, wo_all, wd_y, *refs) = refs[:3], refs[3:]
    if first:
        wo_y, wo_next, x_v, *refs = refs
    else:
        wo_y = w_out
    raw_v, w_v, raw_s, h_v, q_v, k_v, v_v, acc_v, m_v, l_v, o_v, load, h_s, h_r, kv_s, kv_r, y_s, y_r, wo_s, wo_r, o_s, o_r, own_s = refs
    me, r = lax.axis_index('model'), lax.axis_index('resp')
    chip = r // 2
    _, dim, width = w_v.shape
    heads = width // LANES
    log_scale = LOG2E * LANES ** -0.5
    prompt_blocks = k_v.shape[0] - (chunks - 1)

    gather = model_ring(lambda c, b: h_v.at[c, b], h_s, h_r)
    kv = resp_ring(lambda u, b: (k_v, v_v)[u].at[b], kv_s, kv_r)
    ours = ds(r, BLOCK)
    spread = model_ring(lambda u, b: (wd_y, wo_y, wo_next if first else None)[u].at[b], y_s, y_r, lambda u: (w_down, w_out, w_out)[u].at[layer + u // 2, :, ours])
    shares = spread.places[1:]
    outs = resp_ring(lambda u, b: wo_all.at[shares[u], :, ds(b, BLOCK)], wo_s, wo_r, lambda u: wo_y.at[shares[u]])

    raws = [local(w.at[layer], raw_v.at[i], raw_s.at[i]) for i, w in enumerate(heads_in)]

    def x_load(c):
        return pltpu.make_async_copy(xr.at[0, ds(c - 1, BLOCK)], x_v.at[c], load.at[c])

    if first:
        loads = [local(xp, x_v.at[0], load.at[0])]
        for c in range(1, chunks):
            x_load(c).start()
    else:
        loads = [local(h0, h_v.at[0], load.at[0])] + [local(hin.at[c], h_v.at[c, me], load.at[c]) for c in range(1, chunks)]
    greet([gather, kv])

    def own_cols(s):
        return pltpu.make_async_copy(wo_y.at[shares[s]], wo_all.at[shares[s], :, ours], own_s.at[s])

    def start_whole_out():
        for s in range(3):
            outs.start(s)
            own_cols(s).start()

    def key_block(c):
        return jnp.where(c == 0, r, prompt_blocks + c - 1)

    def flatten():
        for i, raw in enumerate(raws):
            raw.wait()

            def part(n):
                w_v[i, ds(n, BLOCK)] = raw_v[i, ds(n, BLOCK)].reshape(BLOCK, width)
            loop(0, dim // BLOCK, part)

    def project(c, then=None):
        rows = pl.ds(pl.multiple_of(c * BLOCK, BLOCK), BLOCK)
        cs, sn = cos[rows, :], sin[rows, :]
        blk = key_block(c)
        for which in range(3):
            if which == 2 and then is not None:
                then()
            for n in range(width // BLOCK):
                y = dot(h_v[c].reshape(BLOCK, dim), w_v[which, :, pl.ds(n * BLOCK, BLOCK)])
                for i in range(2):
                    cols = pl.ds((2 * n + i) * LANES, LANES)
                    part = y[:, i * LANES:(i + 1) * LANES]
                    if which == 1:
                        v_v[blk, cols, :] = part.T.astype(BF)
                    else:
                        part = (part * cs + pltpu.roll(part, LANES // 2, 1) * sn).astype(BF)
                        if which == 2:
                            q_v[c, :, cols] = part
                        else:
                            k_v[blk, :, cols] = part

    def kv_do(*names):
        for name in names:
            for u in range(2):
                getattr(kv, name)(u)

    key_i = lax.broadcasted_iota(jnp.int32, (BLOCK, BLOCK), 0)
    causal = key_i <= lax.broadcasted_iota(jnp.int32, (BLOCK, BLOCK), 1)

    def step(qi, kb, blocks, diagonal=False):
        def scores(n):
            cols = pl.ds(n * LANES, LANES)
            s = dot_t(k_v[pl.ds(kb, blocks), :, cols].reshape(blocks * BLOCK, LANES), q_v[qi, :, cols])
            return jnp.where(causal, s, -jnp.inf) if diagonal else s

        kept = [scores(n) for n in range(heads)]
        tops = [jnp.max(s, axis=0, keepdims=True) for s in kept]
        for n in range(heads):
            s, top = kept[n], tops[n]
            if not diagonal:
                m = m_v[qi, n, :1]
                top = jnp.maximum(m, top)
            p = jnp.exp2((s - top) * log_scale)
            total = jnp.sum(p, axis=0, keepdims=True)
            p = p.astype(BF)
            mixed = None
            for b in range(blocks):
                part = dot(v_v[kb + b, pl.ds(n * LANES, LANES), :], p[b * BLOCK:(b + 1) * BLOCK])
                mixed = part if mixed is None else mixed + part
            if not diagonal:
                alpha = jnp.exp2((m - top) * log_scale)
                total = total + l_v[qi, n, :1] * alpha
                mixed = mixed + acc_v[qi, n] * alpha
            m_v[qi, n, :1] = top
            l_v[qi, n, :1] = total
            acc_v[qi, n] = mixed

    low = 0 if first else 1

    def own(qi):
        step(qi, key_block(qi), 1, True)
        loop(prompt_blocks, prompt_blocks + qi - 1, lambda b: step(qi, b, 1))

    def o_copy(c, k):
        owner = spread.places[k]
        return remote(o_v.at[c, owner], o_out.at[c, :, ds(me, width)], o_s.at[k - 1, c], o_r.at[k - 1, c], 'model', owner)

    def o_own(c):
        return pltpu.make_async_copy(o_v.at[c, me], o_out.at[c, :, ds(me, width)], load.at[c])

    def own_chip(qi):
        when(qi > 0, lambda: step(qi, 2 * chip, 2))
        when((qi == 0) & (r > 2 * chip), lambda: step(qi, 2 * chip, 1))

    def prompt(qi):
        c = qi - low
        if first:
            loop(jnp.where(qi == 0, 4 - chip, 1), 4, lambda x: step(qi, 2 * lax.rem(chip + x, 4), 2))
        else:
            loop(jnp.where(qi == 0, 4, 0), 4, lambda x: step(qi, 2 * x, 2))
        for n in range(heads):
            out = (acc_v[qi, n] / l_v[qi, n, :1]).T.astype(BF)
            o_v[c, :, :, pl.ds(n * LANES, LANES)] = out.reshape(4, ROWS, LANES)
        for k in (2, 1, 3):
            o_copy(c, k).start()
        o_own(c).start()

    def whole_out(*names):
        for name in names:
            for u in range(3):
                getattr(outs, name)(u)

    if first:
        spread.start(1)
        flatten()

        def chunk(c):
            when(c > 0, lambda: x_load(c).wait())
            norm_rows(lambda cols: x_v[c, :, cols], lambda cols, val: h_v.__setitem__((c, slice(None), slice(None), cols), val.reshape(4, ROWS, BLOCK)), gain, BLOCK, dim)
            project(c, lambda: when(c == 0, lambda: kv_do('start')))
            when(c == 1, lambda: (spread.forward(1), spread.start(0)))

        loads[0].wait()
        loop(0, chunks, chunk)

        def own_and_pass(qi):
            own(qi)

            def pass_on():
                kv_do('forward')
                spread.finish(1)
                start_whole_out()
            when(qi == 1, pass_on)

        loop(low, chunks, own_and_pass)
        for u in range(2):
            kv.mate_has(u, OWN_MATE)
        loop(low, chunks, own_chip)
        kv_do('finish')
        spread.forward(0)
        spread.start(2)
        for u in range(2):
            for kind in (LEFT_MATE, RIGHT_MATE, OPP_MATE):
                kv.mate_has(u, kind)

        def prompt_and_events(qi):
            prompt(qi)
            when(qi == 3, lambda: (whole_out('forward'), spread.forward(2)))

        loop(low, chunks, prompt_and_events)
    else:
        for cp in loads:
            cp.wait()
        for c in (1, 2):
            gather.start(c)
        flatten()
        project(jnp.int32(0))
        kv_do('start')

        def chunk(c):
            def receive():
                gather.forward(c)
                when(c + 2 < chunks, lambda: gather.start(c + 2))
            when(c < chunks, receive)
            when(c == 3, lambda: kv_do('finish', 'mate_arrived'))
            when(c == 4, lambda: spread.start(0))
            when(c == 5, lambda: whole_out('forward'))
            when(c >= 3, lambda: prompt(c - 2))

            def use():
                gather.finish(c - 1)
                project(c - 1)
                own(c - 1)
            when((c > 1) & (c <= chunks), use)
            when(c == 2, lambda: (kv_do('forward'), start_whole_out()))
            when(c == 5, lambda: spread.forward(0))

        loop(1, chunks + 2, chunk)
    whole_out('finish')
    spread.finish(0)
    if first:
        spread.finish(2)
    for s in range(3):
        outs.mate_arrived(s)
        outs.drain(s)
        own_cols(s).wait()
    for u in range(2):
        kv.drain(u)
    for u in range(3 if first else 1):
        spread.drain(u)
    for c in range(chunks - low):
        for k in (1, 2, 3):
            o_copy(c, k).wait()
        o_own(c).wait()
    if not first:
        for c in range(1, chunks):
            gather.drain(c)


def attention(first, layer, collective, hidden, gain, cos, sin, heads_in, w_out, w_down):
    _, dim, *by_head = heads_in[0].shape
    width = by_head[0] * by_head[1]
    chunks = cos.shape[0] // BLOCK
    outs = chunks if first else chunks - 1
    heads = width // LANES
    blocks = lax.psum(1, 'resp') + chunks - 1
    tables = ((gain,) if first else ()) + (cos, sin)
    args = (*hidden, *tables, *heads_in, w_out, w_down)
    specs = [ANY] * len(hidden) + [VM] * len(tables) + [ANY] * 5
    ffn = w_down.shape[1]
    shapes = [(outs, ROWS, 4 * width), (4, width, dim), (4, ffn, BLOCK)] + ([(4, width, BLOCK)] * 2 if first else [])
    scratch = [pltpu.VMEM((chunks, BLOCK, dim), BF)] if first else []
    state = pltpu.VMEM((chunks, heads, 8, BLOCK), F32)
    scratch += [
        pltpu.VMEM((3, dim, *by_head), BF),
        pltpu.VMEM((3, dim, width), BF),
        sems(3),
        pltpu.VMEM((chunks, 4, ROWS, dim), BF),
        pltpu.VMEM((chunks, BLOCK, width), BF),
        pltpu.VMEM((blocks, BLOCK, width), BF),
        pltpu.VMEM((blocks, width, BLOCK), BF),
        pltpu.VMEM((chunks, heads, LANES, BLOCK), F32),
        state,
        state,
        pltpu.VMEM((outs, 4, ROWS, width), BF),
        sems(chunks),
    ]
    for kinds, units in ((4, chunks), (8, 2), (4, 3), (8, 3), (3, outs)):
        scratch += [sems(kinds, units)] * 2
    scratch.append(sems(3))
    return pl.pallas_call(
        functools.partial(attention_kernel, first, layer, chunks),
        name=f'attention{layer}',
        out_shape=tuple(jax.ShapeDtypeStruct(s, BF) for s in shapes),
        in_specs=specs,
        out_specs=(ANY,) * len(shapes),
        scratch_shapes=scratch,
        compiler_params=params(collective),
        cost_estimate=work(30_000_000_000),
    )(*args)


def mlp_kernel(first, layer, chunks, *refs):
    o_in, *refs = refs
    count = 2 if first else 1
    rows_in, (gain, next_gain, w_out, wo_all, wg, wu, w_down, wd_y, h_out, h0_out, *refs) = refs[:count], refs[count:]
    if first:
        x_out, *refs = refs
    wo_v, wg_v, wu_v, wd_v, o_v, x_v, u_v, si_v, ri_v, acc_v, hg_v, load, wl, wd_l, wo_l, g_s, g_r, h_s, h_r, x_s, x_r, i_s, i_r = refs
    me, r = lax.axis_index('model'), lax.axis_index('resp')
    dim = x_v.shape[-1]
    ffn = wg_v.shape[0]
    width = wo_v.shape[1]
    rows = chunks * ROWS
    gather = model_ring(lambda c, b: u_v.at[c, b], h_s, h_r)
    shares = gather.places[1:]
    downs = resp_ring(lambda u, b: wd_v.at[u + 1, :, ds(b, BLOCK)], x_s, x_r, lambda u: wd_y.at[shares[u]])
    ahead = model_ring(lambda u, b: hg_v.at[b], g_s, g_r)

    def wo_load(n):
        cols = ds(n, 2 * BLOCK)
        sources = [w_out.at[layer]] + [wo_all.at[s] for s in shares]
        return [pltpu.make_async_copy(src.at[:, cols], wo_v.at[s, :, cols], wo_l.at[i, n]) for i, (s, src) in enumerate(zip(gather.places, sources))]

    start = [local(o_in, o_v, load.at[0])]
    column_loads = dim // (2 * BLOCK)
    loop(0, column_loads, lambda n: [cp.start() for cp in wo_load(n)])
    if first:
        start += [local(rows_in[0].at[ds(me, ROWS)], x_v.at[0], load.at[1])]
        start += [local(rows_in[1].at[0, ds((c - 1) * 4 + me, ROWS)], x_v.at[c], load.at[1 + c]) for c in range(1, chunks)]
    else:
        start += [local(rows_in[0].at[pl.ds(1, chunks)], x_v, load.at[1])]
    greet([gather, downs])
    downs.start(2)
    downs.start(1)
    for cp in start:
        cp.wait()

    def outproj(n):
        cols = ds(n, 2 * BLOCK)
        for cp in wo_load(n):
            cp.wait()
        y = dot(o_v[...].reshape(rows, dim), wo_v[:, :, cols].reshape(dim, 2 * BLOCK))
        x_v[:, :, cols] = (x_v[:, :, cols].reshape(rows, 2 * BLOCK).astype(F32) + y).astype(BF).reshape(chunks, ROWS, 2 * BLOCK)

    loop(0, column_loads, outproj)
    weights = [local(wg.at[layer], wg_v, wl.at[4]), local(wu.at[layer], wu_v, wl.at[5])]
    kept = [local(w_down.at[layer], wd_v.at[0], wd_l.at[0])]
    kept += [local(wd_y.at[s], wd_v.at[i, :, ds(r, BLOCK)], wd_l.at[i]) for i, s in enumerate(shares, 1)]

    def normalize(c):
        norm_rows(lambda cols: x_v[c, :, cols], lambda cols, val: u_v.__setitem__((c, me, slice(None), cols), val), gain, ROWS, dim)
        when(c < 2, lambda: gather.start(c))

    loop(0, chunks, normalize)
    for cp in weights:
        cp.wait()

    def i_send(c, k):
        return remote(si_v.at[c, gather.places[k]], ri_v.at[4 - k, c], i_s.at[k - 1, c], i_r.at[k - 1, c], 'model', gather.places[k])

    def i_recv(c, q):
        ref = ri_v.at[q, c]
        return remote(ref, ref, i_s.at[3 - q, c], i_r.at[3 - q, c], 'model', lax.rem(me + q, 4))

    def gate_up(c):
        lhs = u_v[c].reshape(4 * ROWS, dim)
        half = ffn // 2
        for lo in (0, half):
            cols = pl.ds(lo, half)
            g = dot_t(lhs, wg_v[cols, :])
            inner = (g * jax.nn.sigmoid(g) * dot_t(lhs, wu_v[cols, :])).astype(BF)
            si_v[c, :, :, cols] = inner.reshape(4, ROWS, half)
        for k in (1, 2, 3):
            i_send(c, k).start()
        ri_v[0, c] = si_v[c, me]

    events = {1: lambda: (downs.forward(2), downs.start(0)), 3: lambda: (downs.forward(1), downs.finish(2))}

    def chunk(c):
        def receive():
            gather.forward(c)
            when(c + 2 < chunks, lambda: gather.start(c + 2))
        when(c < chunks, receive)

        def use():
            gather.finish(c - 1)
            gate_up(c - 1)
        when(c > 0, use)
        for at, event in events.items():
            when(c == at, event)

    loop(0, chunks + 1, chunk)
    downs.forward(0)
    downs.finish(1)
    for cp in kept:
        cp.wait()

    def down(lo, hi):
        size = hi - lo
        head = lo == 0
        shape = (size, ROWS, 2 * BLOCK)
        flat = pl.ds(0, size * ROWS)

        def load_rows(n):
            cols = ds(n, 2 * BLOCK)
            acc_v[flat, cols] = x_v[lo:hi, :, cols].reshape(size * ROWS, 2 * BLOCK).astype(F32)

        def store_rows(n):
            cols = ds(n, 2 * BLOCK)
            x_v[lo:hi, :, cols] = acc_v[flat, cols].astype(BF).reshape(shape)

        def product(i):
            q = lax.rem(4 - i, 4)

            def arrive():
                for c in range(lo, hi):
                    i_recv(c, q).wait_recv()
                if head:
                    downs.mate_arrived(q - 1)
            if head:
                when(i == 3, lambda: downs.finish(0))
            else:
                when(i == 2, lambda: ahead.forward(0))
            when(i > 0, arrive)

            def tile(n):
                cols = ds(n, 4 * BLOCK)
                acc_v[flat, cols] = acc_v[flat, cols] + dot(ri_v[q, lo:hi].reshape(size * ROWS, ffn), wd_v[q, :, cols])

            loop(0, dim // (4 * BLOCK), tile)

        loop(0, dim // (2 * BLOCK), load_rows)
        loop(0, 4, product)
        loop(0, dim // (2 * BLOCK), store_rows)
        norm_rows(lambda cols: x_v[lo:hi, :, cols].reshape(size * ROWS, BLOCK), lambda cols, val: o_v.__setitem__((slice(lo, hi), slice(None), cols), val.reshape(size, ROWS, BLOCK)), next_gain, size * ROWS, dim)
        if head:
            hg_v[me] = o_v[0]
            ahead.start(0)
        else:
            ahead.finish(0)

    split = (chunks + 1) // 2
    stored = []
    for part, (lo, hi) in enumerate(((0, split), (split, chunks))):
        down(lo, hi)
        span = pl.ds(lo, hi - lo)
        stored.append(local(o_v.at[span], h_out.at[span], load.at[part]))
        if first:
            stored.append(local(x_v.at[span], x_out.at[span], load.at[2 + part]))
    stored.append(local(hg_v, h0_out, load.at[4]))
    for cp in stored:
        cp.wait()
    ahead.drain(0)
    for u in range(3):
        downs.drain(u)
    for c in range(chunks):
        gather.drain(c)
        for k in (1, 2, 3):
            i_send(c, k).wait_send()


def mlp(first, layer, collective, o_in, rows_in, gain, next_gain, w_out, wo_all, wg, wu, w_down, wd_y):
    chunks, _, dim = o_in.shape
    ffn = wg.shape[1]
    args = (o_in, *rows_in, gain, next_gain, w_out, wo_all, wg, wu, w_down, wd_y)
    specs = [ANY] * (1 + len(rows_in)) + [VM] * 2 + [ANY] * 6
    rows = (chunks, ROWS, dim)
    shapes = [rows, (4, ROWS, dim)] + ([rows] if first else [])
    scratch = [pltpu.VMEM(s, BF) for s in (wo_all.shape, (ffn, dim), (ffn, dim), (4, ffn, dim), (chunks, ROWS, dim), (chunks, ROWS, dim), (chunks, 4, ROWS, dim), (chunks, 4, ROWS, ffn), (4, chunks, ROWS, ffn))]
    scratch += [pltpu.VMEM(((chunks + 1) // 2 * ROWS, dim), F32), pltpu.VMEM((4, ROWS, dim), BF), sems(6), sems(6), sems(4), sems(4, 4)]
    for kinds, units in ((4, 1), (4, chunks), (8, 3), (3, chunks)):
        scratch += [sems(kinds, units)] * 2
    return pl.pallas_call(
        functools.partial(mlp_kernel, first, layer, chunks),
        name=f'mlp{layer}',
        out_shape=tuple(jax.ShapeDtypeStruct(s, BF) for s in shapes),
        in_specs=specs,
        out_specs=(ANY,) * len(shapes),
        scratch_shapes=scratch,
        compiler_params=params(collective),
        cost_estimate=work(80_000_000_000),
    )(*args)


def head_kernel(chunks, tiles, h0, h_in, wv, target, lens, out, wv_v, u_v, even_v, odd_v, m_v, l_v, p_v, t_v, st_v, load, wl, h_s, h_r, st_s, st_r):
    me = lax.axis_index('model')
    dim, vocab = wv_v.shape
    span = vocab // tiles
    tile = 4 * BLOCK
    gather = model_ring(lambda c, b: u_v.at[c, b], h_s, h_r)
    rows = [local(h0, u_v.at[0], load.at[0])] + [local(h_in.at[c], u_v.at[c, me], load.at[c]) for c in range(1, chunks)]

    def weight(t):
        cols = ds(t, span)
        return pltpu.make_async_copy(wv.at[:, cols], wv_v.at[:, cols], wl.at[t])

    weight(0).start()
    greet([gather])
    for cp in rows:
        cp.wait()
    for c in (1, 2):
        gather.start(c)
    lane = lax.broadcasted_iota(jnp.int32, (BLOCK, LANES), 1)
    pieces = range(tile // LANES)
    count = vocab // tile
    per = span // tile

    def logits(c, n):
        return dot(u_v[c].reshape(BLOCK, dim), wv_v[:, ds(n, tile)])

    def reduce_tile(s_v, n):
        parts = [s_v[:, i * LANES:(i + 1) * LANES] for i in pieces]
        m = m_v[...]
        top = functools.reduce(jnp.maximum, parts, m)
        total = l_v[...] * jnp.exp2((m - top) * LOG2E)
        picked = p_v[...]
        wanted = t_v[...] - n * tile
        for i in pieces:
            total = total + jnp.exp2((parts[i] - top) * LOG2E)
            picked = picked + jnp.where(wanted - i * LANES == lane, parts[i], 0.0)
        m_v[...] = top
        l_v[...] = total
        p_v[...] = picked

    def vocab_pass(c):
        m_v[...] = jnp.full_like(m_v, -jnp.inf)
        l_v[...] = jnp.zeros_like(l_v)
        p_v[...] = jnp.zeros_like(p_v)
        t_v[...] = jnp.broadcast_to(target[:, ds(c, BLOCK)], (LANES, BLOCK)).T - me * vocab
        when(c == 0, lambda: (weight(0).wait(), weight(1).start()))
        even_v[...] = logits(c, 0)

        def columns(i):
            n = 2 * i

            def next_weight():
                t = (n + 2) // per
                weight(t).wait()
                when(t + 1 < tiles, lambda: weight(t + 1).start())
            when((c == 0) & (lax.rem(n + 2, per) == 0), next_weight)
            when((i == 1) & (c + 1 < chunks), lambda: pass_on(c + 1))
            odd_v[...] = logits(c, n + 1)
            reduce_tile(even_v, n)
            even_v[...] = logits(c, n + 2)
            reduce_tile(odd_v, n + 1)

        loop(0, count // 2 - 1, columns)
        odd_v[...] = logits(c, count - 1)
        reduce_tile(even_v, count - 2)
        reduce_tile(odd_v, count - 1)
        m = m_v[...]
        top = jnp.max(m, axis=-1, keepdims=True)
        total = jnp.sum(l_v[...] * jnp.exp2((m - top) * LOG2E), axis=-1, keepdims=True)
        picked = jnp.sum(p_v[...], axis=-1, keepdims=True)
        stat = jnp.where(lane == 0, top, jnp.where(lane == 1, total, picked))
        st_v[me, :, ds(c, BLOCK)] = stat.T[:8]

    def pass_on(c):
        gather.forward(c)
        when(c + 2 < chunks, lambda: gather.start(c + 2))

    def chunk(c):
        when(c > 0, lambda: gather.finish(c))
        vocab_pass(c)

    loop(0, chunks, chunk)

    def st_copy(k, block):
        return remote(st_v.at[block], st_v.at[block], st_s.at[k - 1], st_r.at[k - 1], 'model', gather.places[k])

    for k in (2, 1, 3):
        st_copy(k, me).start()
    for k in (1, 2, 3):
        st_copy(k, gather.places[4 - k]).wait_recv()
    tops = [st_v[s, 0:1, :] for s in range(4)]
    top = functools.reduce(jnp.maximum, tops)
    total = sum(st_v[s, 1:2, :] * jnp.exp2((tops[s] - top) * LOG2E) for s in range(4))
    value = sum(st_v[s, 2:3, :] for s in range(4)) - top - jnp.log(total)
    token = lax.broadcasted_iota(jnp.int32, value.shape, 1)
    out[...] = jnp.where(token < lens[0], value, 0.0)
    for k in (1, 2, 3):
        st_copy(k, me).wait_send()
    for c in range(1, chunks):
        gather.drain(c)


def head(collective, h0, h_in, wv, target, lens):
    chunks, _, dim = h_in.shape
    tiles = 4
    stat = pltpu.VMEM((BLOCK, LANES), F32)
    scores = pltpu.VMEM((BLOCK, 4 * BLOCK), F32)
    return pl.pallas_call(
        functools.partial(head_kernel, chunks, tiles),
        name='head',
        out_shape=jax.ShapeDtypeStruct((1, chunks * BLOCK), F32),
        in_specs=[ANY, ANY, ANY, VM, pl.BlockSpec(memory_space=pltpu.SMEM)],
        out_specs=VM,
        scratch_shapes=[
            pltpu.VMEM(wv.shape, BF),
            pltpu.VMEM((chunks, 4, ROWS, dim), BF),
            scores,
            scores,
            stat,
            stat,
            stat,
            pltpu.VMEM((BLOCK, LANES), jnp.int32),
            pltpu.VMEM((4, 8, chunks * BLOCK), F32),
            sems(chunks),
            sems(tiles),
        ] + [sems(4, chunks)] * 2 + [sems(3)] * 2,
        compiler_params=params(collective),
        cost_estimate=work(40_000_000_000),
    )(h0, h_in, wv, target, lens)


def rope_tables(prompt_rows, resp_len, groups):
    half = LANES // 2
    freq = ROPE_BASE ** (-jnp.arange(half, dtype=F32) / half)
    pos = jnp.concatenate([lax.axis_index('resp') * prompt_rows + jnp.arange(prompt_rows), prompt_rows * groups + jnp.arange(resp_len)])
    angles = pos.astype(F32)[:, None] * freq
    c, s = jnp.cos(angles), jnp.sin(angles)
    return jnp.concatenate([c, c], axis=-1), jnp.concatenate([-s, s], axis=-1)


def solution(mesh):
    groups = mesh.shape['resp']
    row_axes = ('prompts', 'resp')
    head_spec = P(None, None, 'model', None)
    in_specs = (P(row_axes, None), P(row_axes, None, None), P(row_axes, None), P(row_axes), P(None, None), head_spec, head_spec, head_spec, P(None, 'model', None, None), P(None, None), P(None, None, 'model'), P(None, None, 'model'), P(None, 'model', None), P(None), P(None, 'model'))

    def device_step(x_prompt, x_resp, targets, resp_lens, attn_gain, w_query, w_key, w_value, w_out, mlp_gain, w_gate, w_up, w_down, final_gain, w_vocab):
        layers, dim, heads, head_dim = w_query.shape
        width = heads * head_dim
        resp_len = x_resp.shape[1]
        cos, sin = rope_tables(x_prompt.shape[0], resp_len, groups)
        w_out = w_out.reshape(layers, width, dim)
        gates = [jnp.swapaxes(w, 1, 2) for w in (w_gate, w_up)]
        gains = [attn_gain[l:l + 1] for l in range(layers)] + [final_gain[None, :]]
        rows = (x_prompt, x_resp)
        hidden = rows
        wo_y = w_out
        for l in range(layers):
            first = l == 0
            o, wo_all, wd_y, *spread = attention(first, l, 2 * l, hidden, gains[l], cos, sin, (w_key, w_value, w_query), wo_y, w_down)
            h, h0, *rows = mlp(first, l, 2 * l + 1, o, rows, mlp_gain[l:l + 1], gains[l + 1], w_out, wo_all, *gates, w_down, wd_y)
            if first:
                wo_y = spread[1]
            hidden = (h0, h)
        return head(2 * layers, h0, h, w_vocab, targets, resp_lens)

    return jax.shard_map(device_step, mesh=mesh, in_specs=in_specs, out_specs=P(row_axes, None), check_vma=False)
```

```python
import functools

import jax
import jax.numpy as jnp
from jax import lax
from jax.experimental import pallas as pl
from jax.experimental.pallas import tpu as pltpu
from jax.sharding import PartitionSpec as P

EPS = 1e-6
ROPE_BASE = 10000.0
LOG2E = 1.4426950408889634
VMEM_BYTES = 67043328
ROWS = 64
LANES = 128
BLOCK = 256
BF = jnp.bfloat16
F32 = jnp.float32
ANY = pl.BlockSpec(memory_space=pl.ANY)
VM = pl.BlockSpec(memory_space=pltpu.VMEM)
MESH = pl.DeviceIdType.MESH
RIGHT, LEFT, RIGHT_ON, LEFT_ON, OWN_MATE, LEFT_MATE, RIGHT_MATE, OPP_MATE = range(8)


def ds(index, size):
    return pl.ds(pl.multiple_of(index * size, size), size)


def dot(a, b):
    return jnp.dot(a, b, preferred_element_type=F32)


def dot_t(a, b):
    return lax.dot_general(a, b, (((1,), (1,)), ((), ())), preferred_element_type=F32)


def sems(*shape):
    return pltpu.SemaphoreType.DMA(shape)


def remote(src, dst, send, recv, axis, where):
    return pltpu.make_async_remote_copy(src_ref=src, dst_ref=dst, send_sem=send, recv_sem=recv, device_id={axis: where}, device_id_type=MESH)


def local(src, dst, sem):
    copy = pltpu.make_async_copy(src, dst, sem)
    copy.start()
    return copy


def greet(rings):
    barrier = pltpu.get_barrier_semaphore()
    peers = {}
    for ring in rings:
        for i, where in enumerate(ring.places[1:]):
            peers[ring.axis, i] = (ring.axis, where)
        if ring.mate is not None:
            peers['mate'] = (ring.axis, ring.mate)
    for axis, where in peers.values():
        pl.semaphore_signal(barrier, inc=1, device_id={axis: where}, device_id_type=MESH)
    pl.semaphore_wait(barrier, len(peers))


class Ring:
    def __init__(self, axis, me, stride, piece, send, recv, source=None, mate=None):
        self.axis, self.piece, self.send, self.recv, self.source, self.mate = axis, piece, send, recv, source, mate
        self.places = [lax.rem(me + k * stride, 4 * stride) for k in range(4)]
        self.own, self.right, self.opp, self.left = self.places
        self.mate_step = None if mate is None else mate - me

    def copy(self, kind, u, owner, source=None):
        dst = self.piece(u, owner)
        if kind in (RIGHT_ON, LEFT_ON):
            half = dst.shape[0] // 2
            dst = dst.at[pl.ds((kind - RIGHT_ON) * half, half)]
        where = self.mate if kind >= OWN_MATE else self.left if kind in (LEFT, LEFT_ON) else self.right
        return remote(dst if source is None else source, dst, self.send.at[kind, u], self.recv.at[kind, u], self.axis, where)

    def start(self, u):
        for kind in (OWN_MATE, RIGHT, LEFT)[self.mate is None:]:
            self.copy(kind, u, self.own, self.source and self.source(u)).start()

    def forward(self, u):
        for kind, owner in ((RIGHT, self.left), (LEFT, self.right)):
            self.copy(kind, u, owner).wait_recv()
            self.copy(kind + RIGHT_ON, u, owner).start()
            if self.mate is not None:
                self.copy(kind + LEFT_MATE, u, owner).start()

    def finish(self, u):
        for kind in (RIGHT_ON, LEFT_ON):
            self.copy(kind, u, self.opp).wait_recv()
        if self.mate is not None:
            self.copy(OPP_MATE, u, self.opp).start()

    def mate_has(self, u, kind):
        owner = {OWN_MATE: self.own, LEFT_MATE: self.left, RIGHT_MATE: self.right, OPP_MATE: self.opp}[kind]
        self.copy(kind, u, owner + self.mate_step).wait_recv()

    def mate_arrived(self, u):
        for kind in range(OWN_MATE, OPP_MATE + 1):
            self.mate_has(u, kind)

    def drain(self, u):
        for kind, owner in ((RIGHT, self.own), (LEFT, self.own), (RIGHT_ON, self.left), (LEFT_ON, self.right), (OWN_MATE, self.own), (LEFT_MATE, self.left), (RIGHT_MATE, self.right), (OPP_MATE, self.opp)):
            if kind < OWN_MATE or self.mate is not None:
                self.copy(kind, u, owner).wait_send()


def resp_ring(piece, send, recv, source=None):
    r = lax.axis_index('resp')
    return Ring('resp', r, 2, piece, send, recv, source, r + 1 - 2 * lax.rem(r, 2))


def model_ring(piece, send, recv, source=None):
    return Ring('model', lax.axis_index('model'), 1, piece, send, recv, source)


def norm_rows(src, dst, gain_ref, rows, width):
    def square(n, total):
        block = src(ds(n, BLOCK)).astype(F32)
        sq = block * block
        return total + sq[:, :LANES] + sq[:, LANES:]

    trips = width // BLOCK
    total = lax.fori_loop(0, trips, square, jnp.zeros((rows, LANES), F32), unroll=2)
    inv = lax.rsqrt(jnp.sum(total, axis=-1, keepdims=True) / width + EPS)

    def scale(n, carry):
        cols = ds(n, BLOCK)
        dst(cols, (src(cols).astype(F32) * inv * gain_ref[:, cols]).astype(BF))
        return carry

    lax.fori_loop(0, trips, scale, 0, unroll=2)


def loop(lo, hi, body):
    def wrapped(i, carry):
        body(i)
        return carry
    lax.fori_loop(lo, hi, wrapped, 0)


def when(condition, *actions):
    @pl.when(condition)
    def _():
        for action in actions:
            action()


def params(collective):
    return pltpu.CompilerParams(collective_id=collective, has_side_effects=True, vmem_limit_bytes=VMEM_BYTES)


def work(flops):
    return pl.CostEstimate(flops=flops, bytes_accessed=flops // 1000, transcendentals=0)


def attention_kernel(first, layer, chunks, *refs):
    if first:
        xp, xr, gain, *refs = refs
    else:
        h0, hin, *refs = refs
    cos, sin, *refs = refs
    heads_in, (w_out, w_down, o_out, wo_all, wd_y, *refs) = refs[:3], refs[3:]
    if first:
        wo_y, wo_next, x_v, *refs = refs
    else:
        wo_y = w_out
    raw_v, w_v, raw_s, h_v, q_v, k_v, v_v, acc_v, m_v, l_v, o_v, load, h_s, h_r, kv_s, kv_r, y_s, y_r, wo_s, wo_r, o_s, o_r, own_s = refs
    me, r = lax.axis_index('model'), lax.axis_index('resp')
    chip = r // 2
    _, dim, width = w_v.shape
    heads = width // LANES
    log_scale = LOG2E * LANES ** -0.5
    prompt_blocks = k_v.shape[0] - (chunks - 1)

    gather = model_ring(lambda c, b: h_v.at[c, b], h_s, h_r)
    kv = resp_ring(lambda u, b: (k_v, v_v)[u].at[b], kv_s, kv_r)
    ours = ds(r, BLOCK)
    half = w_down.shape[1] // 2

    def spread_piece(u, b):
        if u < 2:
            return wd_y.at[b, pl.ds(u * half, half)]
        return (wo_y, wo_next)[u - 2].at[b]

    def spread_source(u):
        if u < 2:
            return w_down.at[layer, pl.ds(u * half, half), ours]
        return w_out.at[u - 2, :, ours]

    spread = model_ring(spread_piece, y_s, y_r, spread_source)
    shares = spread.places[1:]
    outs = resp_ring(lambda u, b: wo_all.at[shares[u], :, ds(b, BLOCK)], wo_s, wo_r, lambda u: wo_y.at[shares[u]])

    for i, w in enumerate(heads_in):
        local(w.at[layer], raw_v.at[i], raw_s.at[i])

    def x_load(c):
        return pltpu.make_async_copy(xr.at[0, ds(c - 1, BLOCK)], x_v.at[c], load.at[c])

    if first:
        loads = [local(xp, x_v.at[0], load.at[0])]
        for c in range(1, chunks):
            x_load(c).start()
    else:
        loads = [local(h0, h_v.at[0], load.at[0])] + [local(hin.at[c], h_v.at[c, me], load.at[c]) for c in range(1, chunks)]
    greet([gather, kv])

    def own_cols(s):
        return pltpu.make_async_copy(wo_y.at[shares[s]], wo_all.at[shares[s], :, ours], own_s.at[s])

    def start_whole_out():
        for s in range(3):
            outs.start(s)
            own_cols(s).start()

    def key_block(c):
        return jnp.where(c == 0, r, prompt_blocks + c - 1)

    def flatten(*which):
        for i in which:
            pltpu.make_async_copy(heads_in[i].at[layer], raw_v.at[i], raw_s.at[i]).wait()

            def part(n):
                w_v[i, ds(n, BLOCK)] = raw_v[i, ds(n, BLOCK)].reshape(BLOCK, width)
            loop(0, dim // BLOCK, part)

    def project(c, then=None, queries=True):
        rows = pl.ds(pl.multiple_of(c * BLOCK, BLOCK), BLOCK)
        cs, sn = cos[rows, :], sin[rows, :]
        blk = key_block(c)
        for which in range(3):
            if which == 2 and then is not None:
                then()
            if which == 2 and not queries:
                continue
            for n in range(width // BLOCK):
                y = dot(h_v[c].reshape(BLOCK, dim), w_v[which, :, pl.ds(n * BLOCK, BLOCK)])
                for i in range(2):
                    cols = pl.ds((2 * n + i) * LANES, LANES)
                    part = y[:, i * LANES:(i + 1) * LANES]
                    if which == 1:
                        v_v[blk, cols, :] = part.T.astype(BF)
                    else:
                        part = (part * cs + pltpu.roll(part, LANES // 2, 1) * sn).astype(BF)
                        if which == 2:
                            q_v[c, :, cols] = part
                        else:
                            k_v[blk, :, cols] = part

    def kv_do(*names):
        for name in names:
            for u in range(2):
                getattr(kv, name)(u)

    key_i = lax.broadcasted_iota(jnp.int32, (BLOCK, BLOCK), 0)
    causal = key_i <= lax.broadcasted_iota(jnp.int32, (BLOCK, BLOCK), 1)

    def step(qi, kb, blocks, diagonal=False):
        def scores(n):
            cols = pl.ds(n * LANES, LANES)
            s = dot_t(k_v[pl.ds(kb, blocks), :, cols].reshape(blocks * BLOCK, LANES), q_v[qi, :, cols]) * log_scale
            return jnp.where(causal, s, -jnp.inf) if diagonal else s

        kept = [scores(n) for n in range(heads)]
        tops = [jnp.max(s, axis=0, keepdims=True) for s in kept]
        for n in range(heads):
            s, top = kept[n], tops[n]
            if not diagonal:
                m = m_v[qi, n, :1]
                top = jnp.maximum(m, top)
            total, mixed = 0.0, 0.0
            for b in range(blocks):
                p = jnp.exp2(s[b * BLOCK:(b + 1) * BLOCK] - top)
                total = total + jnp.sum(p, axis=0, keepdims=True)
                mixed = mixed + dot(v_v[kb + b, pl.ds(n * LANES, LANES), :], p.astype(BF))
            if not diagonal:
                alpha = jnp.exp2(m - top)
                total = total + l_v[qi, n, :1] * alpha
                mixed = mixed + acc_v[qi, n] * alpha
            m_v[qi, n, :1] = top
            l_v[qi, n, :1] = total
            acc_v[qi, n] = mixed

    low = 0 if first else 1

    def own(qi):
        step(qi, key_block(qi), 1, True)
        loop(prompt_blocks, prompt_blocks + qi - 1, lambda b: step(qi, b, 1))

    def o_copy(c, k):
        owner = spread.places[k]
        return remote(o_v.at[c, owner], o_out.at[c, :, ds(me, width)], o_s.at[k - 1, c], o_r.at[k - 1, c], 'model', owner)

    def o_own(c):
        return pltpu.make_async_copy(o_v.at[c, me], o_out.at[c, :, ds(me, width)], load.at[c])

    def own_chip(qi):
        when(qi > 0, lambda: step(qi, 2 * chip, 2))
        when((qi == 0) & (r > 2 * chip), lambda: step(qi, 2 * chip, 1))

    def prompt(qi):
        c = qi - low
        if first:
            side = lax.rem(chip, 2)
            when((qi > 0) | (side == 1), lambda: step(qi, 2 * (chip + 1 - 2 * side), 2))
            when((qi > 0) | (chip > 1), lambda: step(qi, 4 * (1 - chip // 2), 4))
        else:
            loop(0, jnp.where(qi == 0, 0, 2), lambda x: step(qi, 4 * x, 4))
        for n in range(heads):
            out = (acc_v[qi, n] / l_v[qi, n, :1]).T.astype(BF)
            o_v[c, :, :, pl.ds(n * LANES, LANES)] = out.reshape(4, ROWS, LANES)
        for k in (2, 1, 3):
            o_copy(c, k).start()
        o_own(c).start()

    def whole_out(*names):
        for name in names:
            for u in range(3):
                getattr(outs, name)(u)

    if first:
        spread.start(2)
        flatten(0, 1)

        def chunk(c):
            when(c > 0, lambda: x_load(c).wait())
            norm_rows(lambda cols: x_v[c, :, cols], lambda cols, val: h_v.__setitem__((c, slice(None), slice(None), cols), val.reshape(4, ROWS, BLOCK)), gain, BLOCK, dim)
            project(c, lambda: when(c == 0, lambda: (kv_do('start'), flatten(2))))
            when(c == 1, lambda: (spread.forward(2), spread.start(0), spread.start(1)))

        loads[0].wait()
        loop(0, chunks, chunk)

        def own_and_pass(qi):
            own(qi)

            def pass_on():
                kv_do('forward')
                spread.finish(2)
                start_whole_out()
            when(qi == 1, pass_on)

        loop(low, chunks, own_and_pass)
        spread.forward(0)
        for u in range(2):
            kv.mate_has(u, OWN_MATE)
        loop(low, chunks, own_chip)
        kv_do('finish')
        spread.forward(1)
        spread.start(3)
        for u in range(2):
            for kind in (LEFT_MATE, RIGHT_MATE, OPP_MATE):
                kv.mate_has(u, kind)

        def prompt_and_events(qi):
            prompt(qi)
            when(qi == 3, lambda: (whole_out('forward'), spread.forward(3)))

        loop(low, chunks, prompt_and_events)
    else:
        for cp in loads:
            cp.wait()
        for c in (1, 2):
            gather.start(c)
        flatten(0, 1)
        project(jnp.int32(0), queries=False)
        kv_do('start')
        flatten(2)

        def chunk(c):
            def receive():
                gather.forward(c)
                when(c + 2 < chunks, lambda: gather.start(c + 2))
            when(c < chunks, receive)
            when(c == 4, lambda: (spread.start(0), spread.start(1), kv_do('finish', 'mate_arrived')))
            when(c == 5, lambda: spread.forward(0))
            when(c >= 4, lambda: prompt(c - 3))

            def use():
                gather.finish(c - 1)
                project(c - 1)
                own(c - 1)
            when((c > 1) & (c <= chunks), use)
            when(c == 2, lambda: (kv_do('forward'), start_whole_out()))
            when(c == 5, lambda: (whole_out('forward'), spread.forward(1)))

        loop(1, chunks + 3, chunk)
    whole_out('finish')
    for u in (0, 1, 3)[:3 if first else 2]:
        spread.finish(u)
    for s in range(3):
        outs.mate_arrived(s)
        outs.drain(s)
        own_cols(s).wait()
    for u in range(2):
        kv.drain(u)
    for u in range(4 if first else 2):
        spread.drain(u)
    for c in range(chunks - low):
        for k in (1, 2, 3):
            o_copy(c, k).wait()
        o_own(c).wait()
    if not first:
        for c in range(1, chunks):
            gather.drain(c)


def attention(first, layer, collective, hidden, gain, cos, sin, heads_in, w_out, w_down):
    _, dim, *by_head = heads_in[0].shape
    width = by_head[0] * by_head[1]
    chunks = cos.shape[0] // BLOCK
    outs = chunks if first else chunks - 1
    heads = width // LANES
    blocks = lax.psum(1, 'resp') + chunks - 1
    tables = ((gain,) if first else ()) + (cos, sin)
    args = (*hidden, *tables, *heads_in, w_out, w_down)
    specs = [ANY] * len(hidden) + [VM] * len(tables) + [ANY] * 5
    ffn = w_down.shape[1]
    shapes = [(outs, ROWS, 4 * width), (4, width, dim), (4, ffn, BLOCK)] + ([(4, width, BLOCK)] * 2 if first else [])
    scratch = [pltpu.VMEM((chunks, BLOCK, dim), BF)] if first else []
    state = pltpu.VMEM((chunks, heads, 8, BLOCK), F32)
    scratch += [
        pltpu.VMEM((3, dim, *by_head), BF),
        pltpu.VMEM((3, dim, width), BF),
        sems(3),
        pltpu.VMEM((chunks, 4, ROWS, dim), BF),
        pltpu.VMEM((chunks, BLOCK, width), BF),
        pltpu.VMEM((blocks, BLOCK, width), BF),
        pltpu.VMEM((blocks, width, BLOCK), BF),
        pltpu.VMEM((chunks, heads, LANES, BLOCK), F32),
        state,
        state,
        pltpu.VMEM((outs, 4, ROWS, width), BF),
        sems(chunks),
    ]
    for kinds, units in ((4, chunks), (8, 2), (4, 4), (8, 3), (3, outs)):
        scratch += [sems(kinds, units)] * 2
    scratch.append(sems(3))
    return pl.pallas_call(
        functools.partial(attention_kernel, first, layer, chunks),
        name=f'attention{layer}',
        out_shape=tuple(jax.ShapeDtypeStruct(s, BF) for s in shapes),
        in_specs=specs,
        out_specs=(ANY,) * len(shapes),
        scratch_shapes=scratch,
        compiler_params=params(collective),
        cost_estimate=work(30_000_000_000),
    )(*args)


def mlp_kernel(first, layer, chunks, *refs):
    o_in, *refs = refs
    count = 2 if first else 1
    rows_in, (gain, next_gain, w_out, wo_all, wg, wu, w_down, wd_y, h_out, h0_out, *refs) = refs[:count], refs[count:]
    if first:
        x_out, *refs = refs
    wo_v, wg_v, wu_v, wd_v, o_v, x_v, u_v, si_v, ri_v, acc_v, hg_v, load, wl, wd_l, wo_l, g_s, g_r, h_s, h_r, x_s, x_r, i_s, i_r = refs
    me, r = lax.axis_index('model'), lax.axis_index('resp')
    dim = x_v.shape[-1]
    ffn = wg_v.shape[0]
    width = wo_v.shape[1]
    rows = chunks * ROWS
    gather = model_ring(lambda c, b: u_v.at[c, b], h_s, h_r)
    shares = gather.places[1:]
    downs = resp_ring(lambda u, b: wd_v.at[u + 1, :, ds(b, BLOCK)], x_s, x_r, lambda u: wd_y.at[shares[u]])
    ahead = model_ring(lambda u, b: hg_v.at[b], g_s, g_r)

    def wo_load(n):
        cols = ds(n, 2 * BLOCK)
        sources = [w_out.at[layer]] + [wo_all.at[s] for s in shares]
        return [pltpu.make_async_copy(src.at[:, cols], wo_v.at[s, :, cols], wo_l.at[i, n]) for i, (s, src) in enumerate(zip(gather.places, sources))]

    start = [local(o_in, o_v, load.at[0])]
    column_loads = dim // (2 * BLOCK)
    loop(0, column_loads, lambda n: [cp.start() for cp in wo_load(n)])
    if first:
        start += [local(rows_in[0].at[ds(me, ROWS)], x_v.at[0], load.at[1])]
        start += [local(rows_in[1].at[0, ds((c - 1) * 4 + me, ROWS)], x_v.at[c], load.at[1 + c]) for c in range(1, chunks)]
    else:
        start += [local(rows_in[0].at[pl.ds(1, chunks)], x_v, load.at[1])]
    greet([gather, downs])
    downs.start(2)
    downs.start(0)
    for cp in start:
        cp.wait()

    def outproj(n):
        cols = ds(n, 2 * BLOCK)
        for cp in wo_load(n):
            cp.wait()
        y = dot(o_v[...].reshape(rows, dim), wo_v[:, :, cols].reshape(dim, 2 * BLOCK))
        x_v[:, :, cols] = (x_v[:, :, cols].reshape(rows, 2 * BLOCK).astype(F32) + y).astype(BF).reshape(chunks, ROWS, 2 * BLOCK)

    loop(0, column_loads, outproj)
    weights = [local(wg.at[layer], wg_v, wl.at[4]), local(wu.at[layer], wu_v, wl.at[5])]
    kept = [local(w_down.at[layer], wd_v.at[0], wd_l.at[0])]
    kept += [local(wd_y.at[s], wd_v.at[i, :, ds(r, BLOCK)], wd_l.at[i]) for i, s in enumerate(shares, 1)]

    def normalize(c):
        norm_rows(lambda cols: x_v[c, :, cols], lambda cols, val: u_v.__setitem__((c, me, slice(None), cols), val), gain, ROWS, dim)
        when(c < 2, lambda: gather.start(c))

    loop(0, chunks, normalize)
    for cp in weights:
        cp.wait()

    def i_send(c, k):
        return remote(si_v.at[c, gather.places[k]], ri_v.at[4 - k, c], i_s.at[k - 1, c], i_r.at[k - 1, c], 'model', gather.places[k])

    def i_recv(c, q):
        ref = ri_v.at[q, c]
        return remote(ref, ref, i_s.at[3 - q, c], i_r.at[3 - q, c], 'model', lax.rem(me + q, 4))

    def gate_up(c):
        lhs = u_v[c].reshape(4 * ROWS, dim)
        half = ffn // 2
        for lo in (0, half):
            cols = pl.ds(lo, half)
            g = dot_t(lhs, wg_v[cols, :])
            inner = (g * jax.nn.sigmoid(g) * dot_t(lhs, wu_v[cols, :])).astype(BF)
            si_v[c, :, :, cols] = inner.reshape(4, ROWS, half)
        for k in (1, 3, 2):
            i_send(c, k).start()
        ri_v[0, c] = si_v[c, me]

    events = {1: lambda: (downs.forward(2), downs.start(1)), 3: lambda: (downs.forward(0), downs.finish(2))}

    def chunk(c):
        def receive():
            gather.forward(c)
            when(c + 2 < chunks, lambda: gather.start(c + 2))
        when(c < chunks, receive)

        def use():
            gather.finish(c - 1)
            gate_up(c - 1)
        when(c > 0, use)
        for at, event in events.items():
            when(c == at, event)

    loop(0, chunks + 1, chunk)
    downs.forward(1)
    downs.finish(0)
    for cp in kept:
        cp.wait()

    def down(lo, hi):
        size = hi - lo
        head = lo == 0
        shape = (size, ROWS, 2 * BLOCK)
        flat = pl.ds(0, size * ROWS)

        def load_rows(n):
            cols = ds(n, 2 * BLOCK)
            acc_v[flat, cols] = x_v[lo:hi, :, cols].reshape(size * ROWS, 2 * BLOCK).astype(F32)

        def store_rows(n):
            cols = ds(n, 2 * BLOCK)
            x_v[lo:hi, :, cols] = acc_v[flat, cols].astype(BF).reshape(shape)

        def product(i):
            q = jnp.where(i == 1, 3, jnp.maximum(i - 1, 0))

            def arrive():
                for c in range(lo, hi):
                    i_recv(c, q).wait_recv()
                if head:
                    downs.mate_arrived(q - 1)
            if head:
                when(i == 3, lambda: downs.finish(1))
            else:
                when(i == 2, lambda: ahead.forward(0))
            when(i > 0, arrive)

            def tile(n):
                cols = ds(n, 4 * BLOCK)
                acc_v[flat, cols] = acc_v[flat, cols] + dot(ri_v[q, lo:hi].reshape(size * ROWS, ffn), wd_v[q, :, cols])

            loop(0, dim // (4 * BLOCK), tile)

        loop(0, dim // (2 * BLOCK), load_rows)
        loop(0, 4, product)
        loop(0, dim // (2 * BLOCK), store_rows)
        norm_rows(lambda cols: x_v[lo:hi, :, cols].reshape(size * ROWS, BLOCK), lambda cols, val: o_v.__setitem__((slice(lo, hi), slice(None), cols), val.reshape(size, ROWS, BLOCK)), next_gain, size * ROWS, dim)
        if head:
            hg_v[me] = o_v[0]
            ahead.start(0)
        else:
            ahead.finish(0)

    split = (chunks + 1) // 2
    stored = []
    for part, (lo, hi) in enumerate(((0, split), (split, chunks))):
        down(lo, hi)
        span = pl.ds(lo, hi - lo)
        stored.append(local(o_v.at[span], h_out.at[span], load.at[part]))
        if first:
            stored.append(local(x_v.at[span], x_out.at[span], load.at[2 + part]))
    stored.append(local(hg_v, h0_out, load.at[4]))
    for cp in stored:
        cp.wait()
    ahead.drain(0)
    for u in range(3):
        downs.drain(u)
    for c in range(chunks):
        gather.drain(c)
        for k in (1, 2, 3):
            i_send(c, k).wait_send()


def mlp(first, layer, collective, o_in, rows_in, gain, next_gain, w_out, wo_all, wg, wu, w_down, wd_y):
    chunks, _, dim = o_in.shape
    ffn = wg.shape[1]
    args = (o_in, *rows_in, gain, next_gain, w_out, wo_all, wg, wu, w_down, wd_y)
    specs = [ANY] * (1 + len(rows_in)) + [VM] * 2 + [ANY] * 6
    rows = (chunks, ROWS, dim)
    shapes = [rows, (4, ROWS, dim)] + ([rows] if first else [])
    scratch = [pltpu.VMEM(s, BF) for s in (wo_all.shape, (ffn, dim), (ffn, dim), (4, ffn, dim), (chunks, ROWS, dim), (chunks, ROWS, dim), (chunks, 4, ROWS, dim), (chunks, 4, ROWS, ffn), (4, chunks, ROWS, ffn))]
    scratch += [pltpu.VMEM(((chunks + 1) // 2 * ROWS, dim), F32), pltpu.VMEM((4, ROWS, dim), BF), sems(6), sems(6), sems(4), sems(4, 4)]
    for kinds, units in ((4, 1), (4, chunks), (8, 3), (3, chunks)):
        scratch += [sems(kinds, units)] * 2
    return pl.pallas_call(
        functools.partial(mlp_kernel, first, layer, chunks),
        name=f'mlp{layer}',
        out_shape=tuple(jax.ShapeDtypeStruct(s, BF) for s in shapes),
        in_specs=specs,
        out_specs=(ANY,) * len(shapes),
        scratch_shapes=scratch,
        compiler_params=params(collective),
        cost_estimate=work(80_000_000_000),
    )(*args)


def head_kernel(chunks, tiles, h0, h_in, wv, target, lens, out, wv_v, u_v, even_v, odd_v, m_v, l_v, p_v, t_v, st_v, load, wl, h_s, h_r, st_s, st_r):
    me = lax.axis_index('model')
    dim, vocab = wv_v.shape
    span = vocab // tiles
    tile = 4 * BLOCK
    gather = model_ring(lambda c, b: u_v.at[c, b], h_s, h_r)
    rows = [local(h0, u_v.at[0], load.at[0])] + [local(h_in.at[c], u_v.at[c, me], load.at[c]) for c in range(1, chunks)]

    def weight(t):
        cols = ds(t, span)
        return pltpu.make_async_copy(wv.at[:, cols], wv_v.at[:, cols], wl.at[t])

    loop(0, tiles, lambda t: weight(t).start())
    greet([gather])
    for cp in rows:
        cp.wait()
    for c in (1, 2):
        gather.start(c)
    lane = lax.broadcasted_iota(jnp.int32, (BLOCK, LANES), 1)
    pieces = range(tile // LANES)
    count = vocab // tile
    per = span // tile

    def logits(c, n):
        return dot(u_v[c].reshape(BLOCK, dim), wv_v[:, ds(n, tile)])

    def reduce_tile(s_v, n):
        parts = [s_v[:, i * LANES:(i + 1) * LANES] for i in pieces]
        m = m_v[...]
        top = functools.reduce(jnp.maximum, parts, m)
        total = l_v[...] * jnp.exp2((m - top) * LOG2E)
        picked = p_v[...]
        wanted = t_v[...] - n * tile
        for i in pieces:
            total = total + jnp.exp2((parts[i] - top) * LOG2E)
            picked = picked + jnp.where(wanted - i * LANES == lane, parts[i], 0.0)
        m_v[...] = top
        l_v[...] = total
        p_v[...] = picked

    def vocab_pass(c):
        m_v[...] = jnp.full_like(m_v, -jnp.inf)
        l_v[...] = jnp.zeros_like(l_v)
        p_v[...] = jnp.zeros_like(p_v)
        t_v[...] = jnp.broadcast_to(target[:, ds(c, BLOCK)], (LANES, BLOCK)).T - me * vocab
        when(c == 0, lambda: weight(0).wait())
        even_v[...] = logits(c, 0)

        def columns(i):
            n = 2 * i
            when((c == 0) & (lax.rem(n + 2, per) == 0), lambda: weight((n + 2) // per).wait())
            when((i == 1) & (c + 1 < chunks), lambda: pass_on(c + 1))
            odd_v[...] = logits(c, n + 1)
            reduce_tile(even_v, n)
            even_v[...] = logits(c, n + 2)
            reduce_tile(odd_v, n + 1)

        loop(0, count // 2 - 1, columns)
        odd_v[...] = logits(c, count - 1)
        reduce_tile(even_v, count - 2)
        reduce_tile(odd_v, count - 1)
        m = m_v[...]
        top = jnp.max(m, axis=-1, keepdims=True)
        total = jnp.sum(l_v[...] * jnp.exp2((m - top) * LOG2E), axis=-1, keepdims=True)
        picked = jnp.sum(p_v[...], axis=-1, keepdims=True)
        stat = jnp.where(lane == 0, top, jnp.where(lane == 1, total, picked))
        st_v[me, :, ds(c, BLOCK)] = stat.T[:8]

    def pass_on(c):
        gather.forward(c)
        when(c + 2 < chunks, lambda: gather.start(c + 2))

    def chunk(c):
        when(c > 0, lambda: gather.finish(c))
        vocab_pass(c)

    loop(0, chunks, chunk)

    def st_copy(k, block):
        return remote(st_v.at[block], st_v.at[block], st_s.at[k - 1], st_r.at[k - 1], 'model', gather.places[k])

    for k in (2, 1, 3):
        st_copy(k, me).start()
    for k in (1, 2, 3):
        st_copy(k, gather.places[4 - k]).wait_recv()
    tops = [st_v[s, 0:1, :] for s in range(4)]
    top = functools.reduce(jnp.maximum, tops)
    total = sum(st_v[s, 1:2, :] * jnp.exp2((tops[s] - top) * LOG2E) for s in range(4))
    value = sum(st_v[s, 2:3, :] for s in range(4)) - top - jnp.log(total)
    token = lax.broadcasted_iota(jnp.int32, value.shape, 1)
    out[...] = jnp.where(token < lens[0], value, 0.0)
    for k in (1, 2, 3):
        st_copy(k, me).wait_send()
    for c in range(1, chunks):
        gather.drain(c)


def head(collective, h0, h_in, wv, target, lens):
    chunks, _, dim = h_in.shape
    tiles = 4
    stat = pltpu.VMEM((BLOCK, LANES), F32)
    scores = pltpu.VMEM((BLOCK, 4 * BLOCK), F32)
    return pl.pallas_call(
        functools.partial(head_kernel, chunks, tiles),
        name='head',
        out_shape=jax.ShapeDtypeStruct((1, chunks * BLOCK), F32),
        in_specs=[ANY, ANY, ANY, VM, pl.BlockSpec(memory_space=pltpu.SMEM)],
        out_specs=VM,
        scratch_shapes=[
            pltpu.VMEM(wv.shape, BF),
            pltpu.VMEM((chunks, 4, ROWS, dim), BF),
            scores,
            scores,
            stat,
            stat,
            stat,
            pltpu.VMEM((BLOCK, LANES), jnp.int32),
            pltpu.VMEM((4, 8, chunks * BLOCK), F32),
            sems(chunks),
            sems(tiles),
        ] + [sems(4, chunks)] * 2 + [sems(3)] * 2,
        compiler_params=params(collective),
        cost_estimate=work(40_000_000_000),
    )(h0, h_in, wv, target, lens)


def rope_tables(prompt_rows, resp_len, groups):
    half = LANES // 2
    freq = ROPE_BASE ** (-jnp.arange(half, dtype=F32) / half)
    pos = jnp.concatenate([lax.axis_index('resp') * prompt_rows + jnp.arange(prompt_rows), prompt_rows * groups + jnp.arange(resp_len)])
    angles = pos.astype(F32)[:, None] * freq
    c, s = jnp.cos(angles), jnp.sin(angles)
    return jnp.concatenate([c, c], axis=-1), jnp.concatenate([-s, s], axis=-1)


def solution(mesh):
    groups = mesh.shape['resp']
    row_axes = ('prompts', 'resp')
    head_spec = P(None, None, 'model', None)
    in_specs = (P(row_axes, None), P(row_axes, None, None), P(row_axes, None), P(row_axes), P(None, None), head_spec, head_spec, head_spec, P(None, 'model', None, None), P(None, None), P(None, None, 'model'), P(None, None, 'model'), P(None, 'model', None), P(None), P(None, 'model'))

    def device_step(x_prompt, x_resp, targets, resp_lens, attn_gain, w_query, w_key, w_value, w_out, mlp_gain, w_gate, w_up, w_down, final_gain, w_vocab):
        layers, dim, heads, head_dim = w_query.shape
        width = heads * head_dim
        resp_len = x_resp.shape[1]
        cos, sin = rope_tables(x_prompt.shape[0], resp_len, groups)
        w_out = w_out.reshape(layers, width, dim)
        gates = [jnp.swapaxes(w, 1, 2) for w in (w_gate, w_up)]
        gains = [attn_gain[l:l + 1] for l in range(layers)] + [final_gain[None, :]]
        rows = (x_prompt, x_resp)
        hidden = rows
        wo_y = w_out
        for l in range(layers):
            first = l == 0
            o, wo_all, wd_y, *spread = attention(first, l, 2 * l, hidden, gains[l], cos, sin, (w_key, w_value, w_query), wo_y, w_down)
            h, h0, *rows = mlp(first, l, 2 * l + 1, o, rows, mlp_gain[l:l + 1], gains[l + 1], w_out, wo_all, *gates, w_down, wd_y)
            if first:
                wo_y = spread[1]
            hidden = (h0, h)
        return head(2 * layers, h0, h, w_vocab, targets, resp_lens)

    return jax.shard_map(device_step, mesh=mesh, in_specs=in_specs, out_specs=P(row_axes, None), check_vma=False)
```
